32 devices in a mesh: gx: 4 (over z), gy: 4 (over x, core), gz: 2 (over y).
Axes of the slice: x: 2, y: 2, z: 4, core: 2. Of those that a mesh axis runs over, the one named last changes fastest.
Arguments:
- source: float32 [64, 32, 512], P('gx', 'gz', 'gy'), may hold values from -0.6 to 0.6
- shift: float32 [1], replicated, may hold values from 1e-05 to 0.0001
Outputs:
- solution: float32 [64, 32, 512], P('gx', 'gz', 'gy')
The draws below stay inside these ranges and needn't reach their ends.
All inputs are finite; a program needn't handle non-finite values.
Results may differ from the reference program's by a relative error of at most 0.0004.
Values sent between devices are 32-bit elements; how exact they have to be, the bound alone decides.
No kernel may reach another device: no remote copies, remote signals or barrier semaphores. Data moves between devices by JAX's collectives and lax.ppermute only.
A program may use at most 64 MiB of HBM per device.

```python
import math
import jax
import jax.numpy as jnp
from jax import lax

LEVELS = 4
NU_PRE = 1
NU_POST = 1
N0 = 64
N1 = 32
N2 = 512


MEAN_LEVEL = 1e-06


def draw_source(key, part):
    rough_key = jax.random.fold_in(jax.random.fold_in(key, 11), 0)
    rough = jnp.clip(0.1 * jax.random.normal(rough_key, (N0, N1, N2), jnp.float32), -0.59, 0.59)
    return rough - jnp.mean(rough) + MEAN_LEVEL


def setup_inputs(seed: int = 0) -> dict:
    streams_of = jax.random.split(jax.random.key(seed), 3)
    source = draw_source(jax.random.fold_in(streams_of[2], 71), 0)
    shift = jnp.clip(jnp.exp(jax.random.uniform(streams_of[1], (1,), jnp.float32, math.log(9.999999747378752e-06), math.log(0.0001))), 9.999999747378752e-06, 0.0001)
    return {"source": source, "shift": shift}


DAMPING = 6.0 / 7.0
PRECISE = lax.Precision.HIGHEST
CUBIC_EVEN = (-5.0 / 128.0, 35.0 / 128.0, 105.0 / 128.0, -7.0 / 128.0)
CUBIC_ODD = (-7.0 / 128.0, 105.0 / 128.0, 35.0 / 128.0, -5.0 / 128.0)
LINEAR_EVEN = (0.25, 0.75)
LINEAR_ODD = (0.75, 0.25)


def wrapped(values, width):
    return jnp.pad(values, width, mode="wrap")


def neighbours(padded):
    center = padded[1:-1, 1:-1, 1:-1]
    beside_all = padded[2:, 1:-1, 1:-1] + padded[:-2, 1:-1, 1:-1]
    beside_all = beside_all + padded[1:-1, 2:, 1:-1] + padded[1:-1, :-2, 1:-1]
    beside_all = beside_all + padded[1:-1, 1:-1, 2:] + padded[1:-1, 1:-1, :-2]
    return center, beside_all


def defect(padded, forcing, weight_nb, diagonal):
    center, beside_all = neighbours(padded)
    return forcing - (diagonal * center - weight_nb * beside_all)


def relaxed(padded, forcing, weight_nb, diagonal):
    center, beside_all = neighbours(padded)
    return center + DAMPING * (forcing - (diagonal * center - weight_nb * beside_all)) / diagonal


def coarsen(values):
    values = values[0::2] + values[1::2]
    values = values[:, 0::2] + values[:, 1::2]
    values = values[:, :, 0::2] + values[:, :, 1::2]
    return 0.125 * values


def refine_axis(padded, dimension, even_weights, odd_weights):
    margin = len(even_weights) // 2
    length = padded.shape[dimension] - 2 * margin
    even_cells = even_weights[0] * lax.slice_in_dim(padded, 0, length, axis=dimension)
    odd_cells = odd_weights[0] * lax.slice_in_dim(padded, 1, 1 + length, axis=dimension)
    for offset in range(1, len(even_weights)):
        even_cells = even_cells + even_weights[offset] * lax.slice_in_dim(padded, offset, offset + length, axis=dimension)
        odd_cells = odd_cells + odd_weights[offset] * lax.slice_in_dim(padded, offset + 1, offset + 1 + length, axis=dimension)
    stacked = jnp.stack([even_cells, odd_cells], axis=dimension + 1)
    new_shape = list(even_cells.shape)
    new_shape[dimension] = 2 * length
    return stacked.reshape(new_shape)


def refine(padded, even_weights, odd_weights):
    for dimension in range(3):
        padded = refine_axis(padded, dimension, even_weights, odd_weights)
    return padded


def tables(cells_count):
    indices = jnp.arange(cells_count, dtype=jnp.int32)
    angles = ((indices[:, None] * indices[None, :]) % cells_count).astype(jnp.float32) * (2.0 * math.pi / cells_count)
    return jnp.cos(angles), jnp.sin(angles)


def along_axis(matrix, values, dimension):
    product = jnp.tensordot(matrix, values, axes=([1], [dimension]), precision=PRECISE)
    return jnp.moveaxis(product, 0, dimension)


def coarse_solve(forcing, shift_value, weight_nb):
    cosine_table, sine_table = tables(forcing.shape[0])
    real_part = along_axis(cosine_table, forcing, 0)
    imag_part = -along_axis(sine_table, forcing, 0)
    for dimension in (1, 2):
        cosine_table, sine_table = tables(forcing.shape[dimension])
        real_next = along_axis(cosine_table, real_part, dimension) + along_axis(sine_table, imag_part, dimension)
        imag_part = along_axis(cosine_table, imag_part, dimension) - along_axis(sine_table, real_part, dimension)
        real_part = real_next
    cosines = [jnp.cos(jnp.arange(cells_count, dtype=jnp.float32) * (2.0 * math.pi / cells_count)) for cells_count in forcing.shape]
    eigenvalue = weight_nb * (6.0 - 2.0 * cosines[0][:, None, None] - 2.0 * cosines[1][None, :, None] - 2.0 * cosines[2][None, None, :]) + shift_value
    real_part = real_part / eigenvalue
    imag_part = imag_part / eigenvalue
    for dimension in (0, 1):
        cosine_table, sine_table = tables(forcing.shape[dimension])
        real_next = along_axis(cosine_table, real_part, dimension) - along_axis(sine_table, imag_part, dimension)
        imag_part = along_axis(cosine_table, imag_part, dimension) + along_axis(sine_table, real_part, dimension)
        real_part = real_next
    cosine_table, sine_table = tables(forcing.shape[2])
    real_part = along_axis(cosine_table, real_part, 2) - along_axis(sine_table, imag_part, 2)
    return real_part / float(forcing.size)


def vcycle(grid_level, iterate, forcing, shift_value):
    weight_nb = 0.25 ** grid_level
    diagonal = 6.0 * weight_nb + shift_value
    for sweep_index in range(NU_PRE):
        iterate = relaxed(wrapped(iterate, 1), forcing, weight_nb, diagonal)
    residue = coarsen(defect(wrapped(iterate, 1), forcing, weight_nb, diagonal))
    if grid_level + 1 == LEVELS - 1:
        correction = coarse_solve(residue, shift_value, 0.25 ** (grid_level + 1))
    else:
        correction = vcycle(grid_level + 1, jnp.zeros_like(residue), residue, shift_value)
    iterate = iterate + refine(wrapped(correction, 1), LINEAR_EVEN, LINEAR_ODD)
    for sweep_index in range(NU_POST):
        iterate = relaxed(wrapped(iterate, 1), forcing, weight_nb, diagonal)
    return iterate


def reference(source, shift):
    shift_value = shift[0]
    sources = [source]
    for grid_level in range(1, LEVELS):
        sources.append(coarsen(sources[-1]))
    iterate = coarse_solve(sources[-1], shift_value, 0.25 ** (LEVELS - 1))
    for grid_level in range(LEVELS - 2, -1, -1):
        iterate = refine(wrapped(iterate, 2), CUBIC_EVEN, CUBIC_ODD)
        iterate = vcycle(grid_level, iterate, sources[grid_level], shift_value)
    return iterate
```

```python
import math

import jax
import jax.numpy as jnp
from jax import lax
from jax.sharding import PartitionSpec as P

LEVELS = 4


DAMPING = 6.0 / 7.0
PRECISE = lax.Precision.HIGHEST
CUBIC_EVEN = (-5.0 / 128.0, 35.0 / 128.0, 105.0 / 128.0, -7.0 / 128.0)
CUBIC_ODD = (-7.0 / 128.0, 105.0 / 128.0, 35.0 / 128.0, -5.0 / 128.0)
LINEAR_EVEN = (0.25, 0.75)
LINEAR_ODD = (0.75, 0.25)


def extended(block, sides, width):
    for axis, dim in sides:
        count = lax.axis_size(axis)
        forward = [(i, i + 1) for i in range(count - 1)]
        forward.append((count - 1, 0))
        backward = [(target, source) for source, target in forward]
        low = lax.ppermute(
            lax.slice_in_dim(block, block.shape[dim] - width, None, axis=dim), axis, forward
        )
        high = lax.ppermute(lax.slice_in_dim(block, 0, width, axis=dim), axis, backward)
        block = jnp.concatenate([low, block, high], axis=dim)
    return block


def wrapped(values, width):
    return jnp.pad(values, width, mode="wrap")


def neighbours(padded):
    center = padded[1:-1, 1:-1, 1:-1]
    beside_all = padded[2:, 1:-1, 1:-1] + padded[:-2, 1:-1, 1:-1]
    beside_all = beside_all + padded[1:-1, 2:, 1:-1] + padded[1:-1, :-2, 1:-1]
    beside_all = beside_all + padded[1:-1, 1:-1, 2:] + padded[1:-1, 1:-1, :-2]
    return (center, beside_all)


def defect(padded, forcing, weight_nb, diagonal):
    center, beside_all = neighbours(padded)
    return forcing - (diagonal * center - weight_nb * beside_all)


def relaxed(padded, forcing, weight_nb, diagonal):
    center, beside_all = neighbours(padded)
    return center + DAMPING * (forcing - (diagonal * center - weight_nb * beside_all)) / diagonal


def coarsen(values):
    values = values[0::2] + values[1::2]
    values = values[:, 0::2] + values[:, 1::2]
    values = values[:, :, 0::2] + values[:, :, 1::2]
    return 0.125 * values


def refine_axis(padded, dimension, even_weights, odd_weights):
    margin = len(even_weights) // 2
    length = padded.shape[dimension] - 2 * margin
    even_cells = even_weights[0] * lax.slice_in_dim(padded, 0, length, axis=dimension)
    odd_cells = odd_weights[0] * lax.slice_in_dim(padded, 1, 1 + length, axis=dimension)
    for offset in range(1, len(even_weights)):
        even_cells = even_cells + even_weights[offset] * lax.slice_in_dim(
            padded, offset, offset + length, axis=dimension
        )
        odd_cells = odd_cells + odd_weights[offset] * lax.slice_in_dim(
            padded, offset + 1, offset + 1 + length, axis=dimension
        )
    stacked = jnp.stack([even_cells, odd_cells], axis=dimension + 1)
    new_shape = list(even_cells.shape)
    new_shape[dimension] = 2 * length
    return stacked.reshape(new_shape)


def refine(padded, even_weights, odd_weights):
    for dimension in range(3):
        padded = refine_axis(padded, dimension, even_weights, odd_weights)
    return padded


def tables(cells_count):
    indices = jnp.arange(cells_count, dtype=jnp.int32)
    angles = (indices[:, None] * indices[None, :] % cells_count).astype(jnp.float32) * (
        2.0 * math.pi / cells_count
    )
    return (jnp.cos(angles), jnp.sin(angles))


def along_axis(matrix, values, dimension):
    product = jnp.tensordot(matrix, values, axes=([1], [dimension]), precision=PRECISE)
    return jnp.moveaxis(product, 0, dimension)


def coarse_solve(forcing, shift_value, weight_nb):
    cosine_table, sine_table = tables(forcing.shape[0])
    real_part = along_axis(cosine_table, forcing, 0)
    imag_part = -along_axis(sine_table, forcing, 0)
    for dimension in (1, 2):
        cosine_table, sine_table = tables(forcing.shape[dimension])
        real_next = along_axis(cosine_table, real_part, dimension) + along_axis(
            sine_table, imag_part, dimension
        )
        imag_part = along_axis(cosine_table, imag_part, dimension) - along_axis(
            sine_table, real_part, dimension
        )
        real_part = real_next
    cosines = [
        jnp.cos(jnp.arange(cells_count, dtype=jnp.float32) * (2.0 * math.pi / cells_count))
        for cells_count in forcing.shape
    ]
    eigenvalue = (
        weight_nb
        * (
            6.0
            - 2.0 * cosines[0][:, None, None]
            - 2.0 * cosines[1][None, :, None]
            - 2.0 * cosines[2][None, None, :]
        )
        + shift_value
    )
    real_part = real_part / eigenvalue
    imag_part = imag_part / eigenvalue
    for dimension in (0, 1):
        cosine_table, sine_table = tables(forcing.shape[dimension])
        real_next = along_axis(cosine_table, real_part, dimension) - along_axis(
            sine_table, imag_part, dimension
        )
        imag_part = along_axis(cosine_table, imag_part, dimension) + along_axis(
            sine_table, real_part, dimension
        )
        real_part = real_next
    cosine_table, sine_table = tables(forcing.shape[2])
    real_part = along_axis(cosine_table, real_part, 2) - along_axis(sine_table, imag_part, 2)
    return real_part / float(forcing.size)


def vcycle_whole(grid_level, iterate, forcing, shift_value):
    weight_nb = 0.25**grid_level
    diagonal = 6.0 * weight_nb + shift_value
    if iterate is None:
        iterate = DAMPING * forcing / diagonal
    else:
        iterate = relaxed(wrapped(iterate, 1), forcing, weight_nb, diagonal)
    residue = coarsen(defect(wrapped(iterate, 1), forcing, weight_nb, diagonal))
    if grid_level + 1 == LEVELS - 1:
        correction = coarse_solve(residue, shift_value, 0.25 ** (grid_level + 1))
    else:
        correction = vcycle_whole(grid_level + 1, None, residue, shift_value)
    iterate = iterate + refine(wrapped(correction, 1), LINEAR_EVEN, LINEAR_ODD)
    return relaxed(wrapped(iterate, 1), forcing, weight_nb, diagonal)


def collect(block):
    axes = ("gx", "gy", "gz")
    counts = [lax.axis_size(axis) for axis in axes]
    copies = jnp.broadcast_to(block[None], (math.prod(counts),) + block.shape)
    gathered = lax.all_to_all(copies, axes, 0, 0)
    extent_first, extent_second, extent_third = block.shape
    gathered = gathered.reshape(counts + list(block.shape))
    gathered = jnp.transpose(gathered, (0, 3, 2, 4, 1, 5))
    return gathered.reshape(
        counts[0] * extent_first, counts[2] * extent_second, counts[1] * extent_third
    )


def own_block(whole, width, block_shape):
    padded = jnp.pad(whole, width, mode="wrap")
    starts = (
        lax.axis_index("gx") * block_shape[0],
        lax.axis_index("gz") * block_shape[1],
        lax.axis_index("gy") * block_shape[2],
    )
    extents = (block_shape[0] + 2 * width, block_shape[1] + 2 * width, block_shape[2] + 2 * width)
    return lax.dynamic_slice(padded, starts, extents)


def face_halo(block):
    corners = jnp.pad(block, 1)
    for axis, dim in (("gx", 0), ("gy", 2), ("gz", 1)):
        count = lax.axis_size(axis)
        forward = [(i, (i + 1) % count) for i in range(count)]
        backward = [(target, source) for source, target in forward]
        extent = block.shape[dim]
        low = lax.ppermute(
            lax.slice_in_dim(block, extent - 1, None, axis=dim), axis, forward
        )
        high = lax.ppermute(lax.slice_in_dim(block, 0, 1, axis=dim), axis, backward)
        starts = [1, 1, 1]
        starts[dim] = 0
        corners = lax.dynamic_update_slice(corners, low, starts)
        starts[dim] = extent + 1
        corners = lax.dynamic_update_slice(corners, high, starts)
    return corners


def per_device(source, shift):
    shift_value = shift[0]
    source_rim = face_halo(source)
    own_coarse = coarsen(source)
    sources = [None, collect(own_coarse)]
    for grid_level in range(2, LEVELS):
        sources.append(coarsen(sources[-1]))
    whole = coarse_solve(sources[-1], shift_value, 0.25 ** (LEVELS - 1))
    for grid_level in range(LEVELS - 2, 0, -1):
        whole = refine(wrapped(whole, 2), CUBIC_EVEN, CUBIC_ODD)
        whole = vcycle_whole(grid_level, whole, sources[grid_level], shift_value)
    diagonal = 6.0 + shift_value
    iterate = refine(own_block(whole, 3, own_coarse.shape), CUBIC_EVEN, CUBIC_ODD)
    iterate = relaxed(iterate, source_rim, 1.0, diagonal)
    residue = coarsen(defect(iterate, source, 1.0, diagonal))
    correction = vcycle_whole(1, None, collect(residue), shift_value)
    rim = refine(own_block(correction, 2, own_coarse.shape), LINEAR_EVEN, LINEAR_ODD)
    iterate = iterate + rim[1:-1, 1:-1, 1:-1]
    return relaxed(iterate, source, 1.0, diagonal)


def solution(mesh):
    in_specs = (P("gx", "gz", "gy"), P())
    out_specs = P("gx", "gz", "gy")
    return jax.shard_map(
        per_device, mesh=mesh, in_specs=in_specs, out_specs=out_specs, check_vma=False
    )
```

```python
import math

import jax
import jax.numpy as jnp
import numpy as np
from jax import lax
from jax.experimental import pallas as pl
from jax.experimental.pallas import tpu as pltpu
from jax.sharding import PartitionSpec as P

LEVELS = 4


DAMPING = 6.0 / 7.0
PRECISE = lax.Precision.HIGHEST
CUBIC_EVEN = (-5.0 / 128.0, 35.0 / 128.0, 105.0 / 128.0, -7.0 / 128.0)
CUBIC_ODD = (-7.0 / 128.0, 105.0 / 128.0, 35.0 / 128.0, -5.0 / 128.0)
LINEAR_EVEN = (0.25, 0.75)
LINEAR_ODD = (0.75, 0.25)


def extended(block, sides, width):
    for axis, dim in sides:
        count = lax.axis_size(axis)
        forward = [(i, i + 1) for i in range(count - 1)]
        forward.append((count - 1, 0))
        backward = [(target, source) for source, target in forward]
        low = lax.ppermute(
            lax.slice_in_dim(block, block.shape[dim] - width, None, axis=dim), axis, forward
        )
        high = lax.ppermute(lax.slice_in_dim(block, 0, width, axis=dim), axis, backward)
        block = jnp.concatenate([low, block, high], axis=dim)
    return block


def wrapped(values, width):
    return jnp.pad(values, width, mode="wrap")


def neighbours(padded):
    center = padded[1:-1, 1:-1, 1:-1]
    beside_all = padded[2:, 1:-1, 1:-1] + padded[:-2, 1:-1, 1:-1]
    beside_all = beside_all + padded[1:-1, 2:, 1:-1] + padded[1:-1, :-2, 1:-1]
    beside_all = beside_all + padded[1:-1, 1:-1, 2:] + padded[1:-1, 1:-1, :-2]
    return (center, beside_all)


def defect(padded, forcing, weight_nb, diagonal):
    center, beside_all = neighbours(padded)
    return forcing - (diagonal * center - weight_nb * beside_all)


def relaxed(padded, forcing, weight_nb, diagonal):
    center, beside_all = neighbours(padded)
    return center + DAMPING * (forcing - (diagonal * center - weight_nb * beside_all)) / diagonal


def coarsen(values):
    values = values[0::2] + values[1::2]
    values = values[:, 0::2] + values[:, 1::2]
    values = values[:, :, 0::2] + values[:, :, 1::2]
    return 0.125 * values


def refine_axis(padded, dimension, even_weights, odd_weights):
    margin = len(even_weights) // 2
    length = padded.shape[dimension] - 2 * margin
    even_cells = even_weights[0] * lax.slice_in_dim(padded, 0, length, axis=dimension)
    odd_cells = odd_weights[0] * lax.slice_in_dim(padded, 1, 1 + length, axis=dimension)
    for offset in range(1, len(even_weights)):
        even_cells = even_cells + even_weights[offset] * lax.slice_in_dim(
            padded, offset, offset + length, axis=dimension
        )
        odd_cells = odd_cells + odd_weights[offset] * lax.slice_in_dim(
            padded, offset + 1, offset + 1 + length, axis=dimension
        )
    stacked = jnp.stack([even_cells, odd_cells], axis=dimension + 1)
    new_shape = list(even_cells.shape)
    new_shape[dimension] = 2 * length
    return stacked.reshape(new_shape)


def refine(padded, even_weights, odd_weights):
    for dimension in range(3):
        padded = refine_axis(padded, dimension, even_weights, odd_weights)
    return padded


def tables(cells_count):
    indices = jnp.arange(cells_count, dtype=jnp.int32)
    angles = (indices[:, None] * indices[None, :] % cells_count).astype(jnp.float32) * (
        2.0 * math.pi / cells_count
    )
    return (jnp.cos(angles), jnp.sin(angles))


def along_axis(matrix, values, dimension):
    product = jnp.tensordot(matrix, values, axes=([1], [dimension]), precision=PRECISE)
    return jnp.moveaxis(product, 0, dimension)


def coarse_solve(forcing, shift_value, weight_nb):
    cosine_table, sine_table = tables(forcing.shape[0])
    real_part = along_axis(cosine_table, forcing, 0)
    imag_part = -along_axis(sine_table, forcing, 0)
    for dimension in (1, 2):
        cosine_table, sine_table = tables(forcing.shape[dimension])
        real_next = along_axis(cosine_table, real_part, dimension) + along_axis(
            sine_table, imag_part, dimension
        )
        imag_part = along_axis(cosine_table, imag_part, dimension) - along_axis(
            sine_table, real_part, dimension
        )
        real_part = real_next
    cosines = [
        jnp.cos(jnp.arange(cells_count, dtype=jnp.float32) * (2.0 * math.pi / cells_count))
        for cells_count in forcing.shape
    ]
    eigenvalue = (
        weight_nb
        * (
            6.0
            - 2.0 * cosines[0][:, None, None]
            - 2.0 * cosines[1][None, :, None]
            - 2.0 * cosines[2][None, None, :]
        )
        + shift_value
    )
    real_part = real_part / eigenvalue
    imag_part = imag_part / eigenvalue
    for dimension in (0, 1):
        cosine_table, sine_table = tables(forcing.shape[dimension])
        real_next = along_axis(cosine_table, real_part, dimension) - along_axis(
            sine_table, imag_part, dimension
        )
        imag_part = along_axis(cosine_table, imag_part, dimension) + along_axis(
            sine_table, real_part, dimension
        )
        real_part = real_next
    cosine_table, sine_table = tables(forcing.shape[2])
    real_part = along_axis(cosine_table, real_part, 2) - along_axis(sine_table, imag_part, 2)
    return real_part / float(forcing.size)


def vcycle_whole(grid_level, iterate, forcing, shift_value):
    weight_nb = 0.25**grid_level
    diagonal = 6.0 * weight_nb + shift_value
    if iterate is None:
        iterate = DAMPING * forcing / diagonal
    else:
        iterate = relaxed(wrapped(iterate, 1), forcing, weight_nb, diagonal)
    residue = coarsen(defect(wrapped(iterate, 1), forcing, weight_nb, diagonal))
    if grid_level + 1 == LEVELS - 1:
        correction = coarse_solve(residue, shift_value, 0.25 ** (grid_level + 1))
    else:
        correction = vcycle_whole(grid_level + 1, None, residue, shift_value)
    iterate = iterate + refine(wrapped(correction, 1), LINEAR_EVEN, LINEAR_ODD)
    return relaxed(wrapped(iterate, 1), forcing, weight_nb, diagonal)


def collect(block):
    axes = ("gx", "gy", "gz")
    counts = [lax.axis_size(axis) for axis in axes]
    copies = jnp.broadcast_to(block[None], (math.prod(counts),) + block.shape)
    gathered = lax.all_to_all(copies, axes, 0, 0)
    extent_first, extent_second, extent_third = block.shape
    gathered = gathered.reshape(counts + list(block.shape))
    gathered = jnp.transpose(gathered, (0, 3, 2, 4, 1, 5))
    return gathered.reshape(
        counts[0] * extent_first, counts[2] * extent_second, counts[1] * extent_third
    )


def own_block(whole, width, block_shape):
    padded = jnp.pad(whole, width, mode="wrap")
    starts = (
        lax.axis_index("gx") * block_shape[0],
        lax.axis_index("gz") * block_shape[1],
        lax.axis_index("gy") * block_shape[2],
    )
    extents = (block_shape[0] + 2 * width, block_shape[1] + 2 * width, block_shape[2] + 2 * width)
    return lax.dynamic_slice(padded, starts, extents)


def face_halo(block):
    corners = jnp.pad(block, 1)
    for axis, dim in (("gx", 0), ("gy", 2), ("gz", 1)):
        count = lax.axis_size(axis)
        forward = [(i, (i + 1) % count) for i in range(count)]
        backward = [(target, source) for source, target in forward]
        extent = block.shape[dim]
        low = lax.ppermute(
            lax.slice_in_dim(block, extent - 1, None, axis=dim), axis, forward
        )
        high = lax.ppermute(lax.slice_in_dim(block, 0, 1, axis=dim), axis, backward)
        starts = [1, 1, 1]
        starts[dim] = 0
        corners = lax.dynamic_update_slice(corners, low, starts)
        starts[dim] = extent + 1
        corners = lax.dynamic_update_slice(corners, high, starts)
    return corners


def per_device_plain(source, shift):
    shift_value = shift[0]
    source_rim = face_halo(source)
    own_coarse = coarsen(source)
    sources = [None, collect(own_coarse)]
    for grid_level in range(2, LEVELS):
        sources.append(coarsen(sources[-1]))
    whole = coarse_solve(sources[-1], shift_value, 0.25 ** (LEVELS - 1))
    for grid_level in range(LEVELS - 2, 0, -1):
        whole = refine(wrapped(whole, 2), CUBIC_EVEN, CUBIC_ODD)
        whole = vcycle_whole(grid_level, whole, sources[grid_level], shift_value)
    diagonal = 6.0 + shift_value
    iterate = refine(own_block(whole, 3, own_coarse.shape), CUBIC_EVEN, CUBIC_ODD)
    iterate = relaxed(iterate, source_rim, 1.0, diagonal)
    residue = coarsen(defect(iterate, source, 1.0, diagonal))
    correction = vcycle_whole(1, None, collect(residue), shift_value)
    rim = refine(own_block(correction, 2, own_coarse.shape), LINEAR_EVEN, LINEAR_ODD)
    iterate = iterate + rim[1:-1, 1:-1, 1:-1]
    return relaxed(iterate, source, 1.0, diagonal)


def halving(count):
    matrix = np.zeros((count // 2, count))
    for cell in range(count):
        matrix[cell // 2, cell] = 1.0
    return matrix


def doubling(cells, count, even_weights, odd_weights, start=0, periodic=True):
    matrix = np.zeros((len(cells), count))
    margin = len(even_weights) // 2
    for row, cell in enumerate(cells):
        if cell is None:
            continue
        weights = odd_weights if cell % 2 else even_weights
        first = cell // 2 - margin + cell % 2
        for offset, weight in enumerate(weights):
            column = first + offset - start
            matrix[row, column % count if periodic else column] += weight
    return matrix


def pieces(matrix):
    rest = np.asarray(matrix, np.float64)
    found = []
    while np.any(rest) and len(found) < 3:
        part = rest.astype(jnp.bfloat16)
        found.append(part)
        rest = rest - part.astype(np.float64)
    return found


def ring_cells(extent, total, margin):
    cells = [None] * total
    for cell in range(-margin, extent + margin):
        cells[cell % total] = cell
    return cells


def split_values(values):
    high = values.astype(jnp.bfloat16)
    rest = values - high.astype(jnp.float32)
    middle = rest.astype(jnp.bfloat16)
    low = (rest - middle.astype(jnp.float32)).astype(jnp.bfloat16)
    return (low, middle, high)


def from_left(matrix_refs, values):
    total = None
    parts = split_values(values)
    for matrix_ref in reversed(matrix_refs):
        for part in parts:
            term = jnp.dot(matrix_ref[...], part, preferred_element_type=jnp.float32)
            total = term if total is None else total + term
    return total


def from_right(values, matrix_refs):
    total = None
    parts = split_values(values)
    for matrix_ref in reversed(matrix_refs):
        for part in parts:
            term = jnp.dot(part, matrix_ref[...], preferred_element_type=jnp.float32)
            total = term if total is None else total + term
    return total


def flat(values):
    return values.reshape(values.shape[0] * values.shape[1], values.shape[2])


def beside_rolled(values, periodic_first):
    if periodic_first:
        total = jnp.concatenate([values[1:], values[:1]], axis=0) + jnp.concatenate(
            [values[-1:], values[:-1]], axis=0
        )
        center = values
    else:
        total = values[2:] + values[:-2]
        center = values[1:-1]
    for axis in (1, 2):
        extent = values.shape[axis]
        total = total + (pltpu.roll(center, 1, axis) + pltpu.roll(center, extent - 1, axis))
    return (center, total)


def defect_rolled(values, forcing, weight_nb, diagonal, periodic_first=True):
    center, total = beside_rolled(values, periodic_first)
    return forcing - (diagonal * center - weight_nb * total)


def damping_over(diagonal, extent):
    return jnp.full((1, 1, extent), DAMPING, jnp.float32) / diagonal


def sweep_rolled(values, forcing, weight_nb, diagonal, periodic_first=True):
    center, total = beside_rolled(values, periodic_first)
    scale = damping_over(diagonal, values.shape[2])
    return center + scale * (forcing - (diagonal * center - weight_nb * total))


def level_tables(grid_level, shape):
    first, second, third = shape
    found = {}
    found["rows_down"] = pieces(np.kron(halving(first), halving(second)))
    found["lanes_down"] = pieces(0.125 * halving(third).T)
    for name, even, odd in (
        ("linear", LINEAR_EVEN, LINEAR_ODD),
        ("cubic", CUBIC_EVEN, CUBIC_ODD),
    ):
        up = [doubling(range(count), count // 2, even, odd) for count in shape]
        found["rows_" + name] = pieces(np.kron(up[0], up[1]))
        found["lanes_" + name] = pieces(up[2].T)
    return {(grid_level, name): value for name, value in found.items()}


def solve_tables(shape):
    def hartley(count):
        indices = np.arange(count)
        angles = 2.0 * np.pi * (indices[:, None] * indices[None, :] % count) / count
        return np.cos(angles) + np.sin(angles)

    cosines = [np.cos(2.0 * np.pi * np.arange(count) / count) for count in shape]
    spread = (
        6.0
        - 2.0 * cosines[0][:, None, None]
        - 2.0 * cosines[1][None, :, None]
        - 2.0 * cosines[2][None, None, :]
    )
    spread = 0.25 ** (LEVELS - 1) * spread.reshape(shape[0] * shape[1], shape[2])
    rows = np.kron(hartley(shape[0]), hartley(shape[1]))
    return {
        ("solve", "rows"): [rows.astype(np.float32)],
        ("solve", "lanes"): [hartley(shape[2]).astype(np.float32)],
        ("solve", "spread"): [spread.astype(np.float32)],
    }


def solve_rolled(tables_of, forcing, shift_value):
    rows = tables_of["solve", "rows"][0][...]
    lanes = tables_of["solve", "lanes"][0][...]

    def transform(values):
        values = jnp.dot(rows, values, precision=PRECISE, preferred_element_type=jnp.float32)
        return jnp.dot(values, lanes, precision=PRECISE, preferred_element_type=jnp.float32)

    modes = transform(forcing) / (tables_of["solve", "spread"][0][...] + shift_value)
    return transform(modes) * (1.0 / forcing.size)


def down(tables_of, grid_level, values):
    coarse = from_left(tables_of[grid_level, "rows_down"], flat(values))
    return from_right(coarse, tables_of[grid_level, "lanes_down"])


def up(tables_of, grid_level, name, values, shape):
    wide = from_right(values, tables_of[grid_level, "lanes_" + name])
    return from_left(tables_of[grid_level, "rows_" + name], wide).reshape(shape)


def vcycle_rolled(tables_of, grid_level, iterate, forcing, shift_value):
    weight_nb = 0.25**grid_level
    diagonal = 6.0 * weight_nb + shift_value
    shape = forcing.shape
    if iterate is None:
        iterate = damping_over(diagonal, shape[2]) * forcing
    else:
        iterate = sweep_rolled(iterate, forcing, weight_nb, diagonal)
    residue = down(tables_of, grid_level, defect_rolled(iterate, forcing, weight_nb, diagonal))
    if grid_level + 1 == LEVELS - 1:
        correction = solve_rolled(tables_of, residue, shift_value)
    else:
        coarse_shape = tuple(extent // 2 for extent in shape)
        correction = flat(
            vcycle_rolled(
                tables_of, grid_level + 1, None, residue.reshape(coarse_shape), shift_value
            )
        )
    iterate = iterate + up(tables_of, grid_level, "linear", correction, shape)
    return sweep_rolled(iterate, forcing, weight_nb, diagonal)


def pack(tables_of, values):
    coarse = from_left(tables_of["own", "rows_down"], flat(values))
    half = coarse.shape[0] // 2
    return from_right(coarse[:half], tables_of["own", "left_down"]) + from_right(
        coarse[half:], tables_of["own", "right_down"]
    )


def unpack(gathered_ref, whole_ref, counts, extents):
    half, second, lanes = (extents[0] // 2, extents[1], 2 * extents[2])
    low_lane = lax.broadcasted_iota(jnp.int32, (half, second, lanes), 2) < extents[2]
    for x in range(counts[0]):
        for z in range(counts[2]):
            for pair in range(counts[1] // 2):
                blocks = [
                    gathered_ref[(x * counts[1] + 2 * pair + side) * counts[2] + z].reshape(
                        half, second, lanes
                    )
                    for side in range(2)
                ]
                turned = [pltpu.roll(block, extents[2], 2) for block in blocks]
                window = (pl.ds(z * second, second), pl.ds(pair * lanes, lanes))
                whole_ref[(pl.ds(x * 2 * half, half), *window)] = jnp.where(
                    low_lane, blocks[0], turned[1]
                )
                whole_ref[(pl.ds(x * 2 * half + half, half), *window)] = jnp.where(
                    low_lane, turned[0], blocks[1]
                )


def own_window(whole, scratch_ref, margin, extents, place_ref):
    count = whole.shape[0]
    scratch_ref[pl.ds(margin, count)] = whole
    scratch_ref[pl.ds(0, margin)] = whole[count - margin :]
    scratch_ref[pl.ds(margin + count, margin)] = whole[:margin]
    cut = scratch_ref[pl.ds(place_ref[0] * extents[0], extents[0] + 2 * margin)]
    turn_second = (whole.shape[1] - place_ref[1] * extents[1]) % whole.shape[1]
    turn_third = (whole.shape[2] - place_ref[2] * extents[2]) % whole.shape[2]
    return pltpu.roll(pltpu.roll(cut, turn_second, 1), turn_third, 2)


def with_tables(body, tables_map, n_plain):
    keys = [(key, len(value)) for key, value in tables_map.items()]
    arrays = [jnp.asarray(part) for value in tables_map.values() for part in value]

    def kernel(*refs):
        position = n_plain
        tables_of = {}
        for key, length in keys:
            tables_of[key] = refs[position : position + length]
            position += length
        body(tables_of, refs[:n_plain], refs[position:])

    return (kernel, arrays)


def per_device_kernels(source, shift):
    counts = tuple(lax.axis_size(axis) for axis in ("gx", "gy", "gz"))
    block = source.shape
    extents = tuple(extent // 2 for extent in block)
    shape = (extents[0] * counts[0], extents[1] * counts[2], extents[2] * counts[1])
    place = jnp.stack([lax.axis_index("gx"), lax.axis_index("gz"), lax.axis_index("gy")])
    devices = math.prod(counts)
    rows_wide = block[1] + 8
    lanes_wide = 2 * block[2]
    vmem = pl.BlockSpec(memory_space=pltpu.VMEM)
    smem = pl.BlockSpec(memory_space=pltpu.SMEM)

    own = {("own", "rows_down"): pieces(np.kron(halving(block[0]), halving(block[1])))}
    narrow = 0.125 * halving(block[2]).T
    own["own", "left_down"] = pieces(np.concatenate([narrow, 0.0 * narrow], axis=1))
    own["own", "right_down"] = pieces(np.concatenate([0.0 * narrow, narrow], axis=1))

    def edge_tables(name, even, odd, margin):
        fine = margin
        coarse = len(even) // 2 + 1
        first = doubling(
            range(-fine, block[0] + fine), extents[0] + 2 * coarse, even, odd, -coarse, False
        )
        second = doubling(ring_cells(block[1], rows_wide, fine), shape[1], even, odd)
        third = doubling(ring_cells(block[2], lanes_wide, fine), shape[2], even, odd)
        return {
            ("own", "rows_" + name): pieces(np.kron(first, second)),
            ("own", "lanes_" + name): pieces(third.T),
        }

    levels = {}
    for grid_level in range(1, LEVELS - 1):
        levels.update(
            level_tables(grid_level, tuple(extent >> (grid_level - 1) for extent in shape))
        )
    levels.update(solve_tables(tuple(extent >> (LEVELS - 2) for extent in shape)))

    def gather(copies):
        return lax.all_to_all(copies, ("gx", "gy", "gz"), 0, 0)

    copies_shape = jax.ShapeDtypeStruct(
        (devices, extents[0] // 2 * extents[1], 2 * extents[2]), jnp.float32
    )

    def pack_body(tables_of, ins, outs):
        outs[0][...] = jnp.broadcast_to(pack(tables_of, ins[0][...])[None], copies_shape.shape)

    kernel, arrays = with_tables(pack_body, own, 1)
    copies = pl.pallas_call(
        kernel,
        out_shape=copies_shape,
        in_specs=[vmem] * (1 + len(arrays)),
        out_specs=vmem,
        name="pack",
    )(source, *arrays)

    rims = []
    for axis, dim in (("gx", 0), ("gz", 1), ("gy", 2)):
        count = lax.axis_size(axis)
        forward = [(i, (i + 1) % count) for i in range(count)]
        backward = [(target, origin) for origin, target in forward]
        rims.append(
            lax.ppermute(
                lax.slice_in_dim(source, block[dim] - 1, None, axis=dim), axis, forward
            )
        )
        rims.append(lax.ppermute(lax.slice_in_dim(source, 0, 1, axis=dim), axis, backward))
    gathered = gather(copies)

    def first_body(tables_of, ins, outs):
        shift_ref, place_ref, gathered_ref, source_ref = ins[:4]
        low_first, high_first, low_second, high_second, low_third, high_third = ins[4:]
        copies_ref, iterate_ref, whole_ref, scratch_ref = outs
        shift_value = shift_ref[0]
        unpack(gathered_ref, whole_ref, counts, extents)
        whole_forcing = whole_ref[...]
        forcings = [whole_forcing]
        for grid_level in range(1, LEVELS - 1):
            fine = forcings[-1]
            coarse = down(tables_of, grid_level, fine)
            if grid_level + 1 < LEVELS - 1:
                coarse = coarse.reshape(tuple(extent // 2 for extent in fine.shape))
            forcings.append(coarse)
        iterate = solve_rolled(tables_of, forcings[-1], shift_value)
        for grid_level in range(LEVELS - 2, 0, -1):
            forcing = forcings[grid_level - 1]
            if iterate.ndim == 3:
                iterate = flat(iterate)
            iterate = up(tables_of, grid_level, "cubic", iterate, forcing.shape)
            iterate = vcycle_rolled(tables_of, grid_level, iterate, forcing, shift_value)
        window = own_window(iterate, scratch_ref, 3, extents, place_ref)
        iterate = from_right(flat(window), tables_of["own", "lanes_cubic"])
        iterate = from_left(tables_of["own", "rows_cubic"], iterate)
        iterate = iterate.reshape(block[0] + 4, rows_wide, lanes_wide)

        wide = (block[0], rows_wide, lanes_wide)
        row = lax.broadcasted_iota(jnp.int32, wide, 1)
        lane = lax.broadcasted_iota(jnp.int32, wide, 2)

        def widened(values):
            first = values.shape[0]
            values = jnp.concatenate([values, jnp.zeros_like(values[:, :8])], axis=1)
            return jnp.concatenate([values, jnp.zeros((first, rows_wide, block[2]))], axis=2)

        def rows_only(values):
            values = jnp.concatenate([values, jnp.zeros_like(values)], axis=2)
            return jnp.broadcast_to(values, wide)

        def lanes_only(values):
            values = jnp.broadcast_to(values, (block[0], block[1], lanes_wide))
            return jnp.concatenate([values, jnp.zeros_like(values[:, :8])], axis=1)

        middle = widened(source_ref[...])
        middle = jnp.where(row == block[1], rows_only(high_second[...]), middle)
        middle = jnp.where(row == rows_wide - 1, rows_only(low_second[...]), middle)
        middle = jnp.where(lane == block[2], lanes_only(high_third[...]), middle)
        middle = jnp.where(lane == lanes_wide - 1, lanes_only(low_third[...]), middle)
        forcing = jnp.concatenate(
            [widened(low_first[...]), middle, widened(high_first[...])], axis=0
        )
        diagonal = 6.0 + shift_value
        iterate = sweep_rolled(iterate, forcing, 1.0, diagonal, False)
        iterate_ref[...] = iterate
        residue = defect_rolled(iterate, middle, 1.0, diagonal, False)
        packed = pack(tables_of, residue[:, : block[1], : block[2]])
        copies_ref[...] = jnp.broadcast_to(packed[None], copies_ref.shape)

    tables_map = {**levels, **own, **edge_tables("cubic", CUBIC_EVEN, CUBIC_ODD, 2)}
    kernel, arrays = with_tables(first_body, tables_map, 10)
    iterate_shape = jax.ShapeDtypeStruct((block[0] + 2, rows_wide, lanes_wide), jnp.float32)
    copies, iterate = pl.pallas_call(
        kernel,
        out_shape=(copies_shape, iterate_shape),
        in_specs=[smem, smem] + [vmem] * (8 + len(arrays)),
        out_specs=(vmem, vmem),
        scratch_shapes=[
            pltpu.VMEM(shape, jnp.float32),
            pltpu.VMEM((shape[0] + 6, *shape[1:]), jnp.float32),
        ],
        name="first",
    )(shift, place, gathered, source, *rims, *arrays)
    gathered = gather(copies)

    def second_body(tables_of, ins, outs):
        shift_ref, place_ref, gathered_ref, source_ref, iterate_ref = ins
        result_ref, whole_ref, scratch_ref = outs
        shift_value = shift_ref[0]
        unpack(gathered_ref, whole_ref, counts, extents)
        correction = vcycle_rolled(tables_of, 1, None, whole_ref[...], shift_value)
        window = own_window(correction, scratch_ref, 2, extents, place_ref)
        wide = from_right(flat(window), tables_of["own", "lanes_linear"])
        wide = from_left(tables_of["own", "rows_linear"], wide).reshape(iterate_shape.shape)
        iterate = iterate_ref[...] + wide
        center, total = beside_rolled(iterate, False)
        center = center[:, : block[1], : block[2]]
        total = total[:, : block[1], : block[2]]
        diagonal = 6.0 + shift_value
        scale = damping_over(diagonal, block[2])
        result_ref[...] = center + scale * (source_ref[...] - (diagonal * center - total))

    tables_map = {key: value for key, value in levels.items() if "cubic" not in key[1]}
    tables_map.update(edge_tables("linear", LINEAR_EVEN, LINEAR_ODD, 1))
    kernel, arrays = with_tables(second_body, tables_map, 5)
    return pl.pallas_call(
        kernel,
        out_shape=jax.ShapeDtypeStruct(block, jnp.float32),
        in_specs=[smem, smem] + [vmem] * (3 + len(arrays)),
        out_specs=vmem,
        scratch_shapes=[
            pltpu.VMEM(shape, jnp.float32),
            pltpu.VMEM((shape[0] + 4, *shape[1:]), jnp.float32),
        ],
        name="second",
    )(shift, place, gathered, source, iterate, *arrays)


WHOLE_LIMIT = 1 << 18


def per_device(source, shift):
    block = source.shape
    counts = tuple(lax.axis_size(axis) for axis in ("gx", "gy", "gz"))
    cells = math.prod(block) // 8 * math.prod(counts)
    second_deep = block[1] * counts[2] >> (LEVELS - 2)
    third_deep = block[2] * counts[1] >> (LEVELS - 2)
    aligned = (
        block[0] % 4 == 0
        and block[1] % 16 == 0
        and block[2] == 128
        and counts[1] % 2 == 0
        and second_deep % 8 == 0
        and third_deep % 128 == 0
        and block[0] * counts[0] >= 32
    )
    if aligned and cells <= WHOLE_LIMIT:
        return per_device_kernels(source, shift)
    return per_device_plain(source, shift)


def solution(mesh):
    in_specs = (P("gx", "gz", "gy"), P())
    out_specs = P("gx", "gz", "gy")
    return jax.shard_map(
        per_device, mesh=mesh, in_specs=in_specs, out_specs=out_specs, check_vma=False
    )
```

```python
import math

import jax
import jax.numpy as jnp
import numpy as np
from jax import lax
from jax.experimental import pallas as pl
from jax.experimental.pallas import tpu as pltpu
from jax.sharding import PartitionSpec as P

LEVELS = 4


DAMPING = 6.0 / 7.0
PRECISE = lax.Precision.HIGHEST
CUBIC_EVEN = (-5.0 / 128.0, 35.0 / 128.0, 105.0 / 128.0, -7.0 / 128.0)
CUBIC_ODD = (-7.0 / 128.0, 105.0 / 128.0, 35.0 / 128.0, -5.0 / 128.0)
LINEAR_EVEN = (0.25, 0.75)
LINEAR_ODD = (0.75, 0.25)


def extended(block, sides, width):
    for axis, dim in sides:
        count = lax.axis_size(axis)
        forward = [(i, i + 1) for i in range(count - 1)]
        forward.append((count - 1, 0))
        backward = [(target, source) for source, target in forward]
        low = lax.ppermute(
            lax.slice_in_dim(block, block.shape[dim] - width, None, axis=dim), axis, forward
        )
        high = lax.ppermute(lax.slice_in_dim(block, 0, width, axis=dim), axis, backward)
        block = jnp.concatenate([low, block, high], axis=dim)
    return block


def wrapped(values, width):
    return jnp.pad(values, width, mode="wrap")


def neighbours(padded):
    center = padded[1:-1, 1:-1, 1:-1]
    beside_all = padded[2:, 1:-1, 1:-1] + padded[:-2, 1:-1, 1:-1]
    beside_all = beside_all + padded[1:-1, 2:, 1:-1] + padded[1:-1, :-2, 1:-1]
    beside_all = beside_all + padded[1:-1, 1:-1, 2:] + padded[1:-1, 1:-1, :-2]
    return (center, beside_all)


def defect(padded, forcing, weight_nb, diagonal):
    center, beside_all = neighbours(padded)
    return forcing - (diagonal * center - weight_nb * beside_all)


def relaxed(padded, forcing, weight_nb, diagonal):
    center, beside_all = neighbours(padded)
    return center + DAMPING * (forcing - (diagonal * center - weight_nb * beside_all)) / diagonal


def coarsen(values):
    values = values[0::2] + values[1::2]
    values = values[:, 0::2] + values[:, 1::2]
    values = values[:, :, 0::2] + values[:, :, 1::2]
    return 0.125 * values


def refine_axis(padded, dimension, even_weights, odd_weights):
    margin = len(even_weights) // 2
    length = padded.shape[dimension] - 2 * margin
    even_cells = even_weights[0] * lax.slice_in_dim(padded, 0, length, axis=dimension)
    odd_cells = odd_weights[0] * lax.slice_in_dim(padded, 1, 1 + length, axis=dimension)
    for offset in range(1, len(even_weights)):
        even_cells = even_cells + even_weights[offset] * lax.slice_in_dim(
            padded, offset, offset + length, axis=dimension
        )
        odd_cells = odd_cells + odd_weights[offset] * lax.slice_in_dim(
            padded, offset + 1, offset + 1 + length, axis=dimension
        )
    stacked = jnp.stack([even_cells, odd_cells], axis=dimension + 1)
    new_shape = list(even_cells.shape)
    new_shape[dimension] = 2 * length
    return stacked.reshape(new_shape)


def refine(padded, even_weights, odd_weights):
    for dimension in range(3):
        padded = refine_axis(padded, dimension, even_weights, odd_weights)
    return padded


def tables(cells_count):
    indices = jnp.arange(cells_count, dtype=jnp.int32)
    angles = (indices[:, None] * indices[None, :] % cells_count).astype(jnp.float32) * (
        2.0 * math.pi / cells_count
    )
    return (jnp.cos(angles), jnp.sin(angles))


def along_axis(matrix, values, dimension):
    product = jnp.tensordot(matrix, values, axes=([1], [dimension]), precision=PRECISE)
    return jnp.moveaxis(product, 0, dimension)


def coarse_solve(forcing, shift_value, weight_nb):
    cosine_table, sine_table = tables(forcing.shape[0])
    real_part = along_axis(cosine_table, forcing, 0)
    imag_part = -along_axis(sine_table, forcing, 0)
    for dimension in (1, 2):
        cosine_table, sine_table = tables(forcing.shape[dimension])
        real_next = along_axis(cosine_table, real_part, dimension) + along_axis(
            sine_table, imag_part, dimension
        )
        imag_part = along_axis(cosine_table, imag_part, dimension) - along_axis(
            sine_table, real_part, dimension
        )
        real_part = real_next
    cosines = [
        jnp.cos(jnp.arange(cells_count, dtype=jnp.float32) * (2.0 * math.pi / cells_count))
        for cells_count in forcing.shape
    ]
    eigenvalue = (
        weight_nb
        * (
            6.0
            - 2.0 * cosines[0][:, None, None]
            - 2.0 * cosines[1][None, :, None]
            - 2.0 * cosines[2][None, None, :]
        )
        + shift_value
    )
    real_part = real_part / eigenvalue
    imag_part = imag_part / eigenvalue
    for dimension in (0, 1):
        cosine_table, sine_table = tables(forcing.shape[dimension])
        real_next = along_axis(cosine_table, real_part, dimension) - along_axis(
            sine_table, imag_part, dimension
        )
        imag_part = along_axis(cosine_table, imag_part, dimension) + along_axis(
            sine_table, real_part, dimension
        )
        real_part = real_next
    cosine_table, sine_table = tables(forcing.shape[2])
    real_part = along_axis(cosine_table, real_part, 2) - along_axis(sine_table, imag_part, 2)
    return real_part / float(forcing.size)


def vcycle_whole(grid_level, iterate, forcing, shift_value):
    weight_nb = 0.25**grid_level
    diagonal = 6.0 * weight_nb + shift_value
    if iterate is None:
        iterate = DAMPING * forcing / diagonal
    else:
        iterate = relaxed(wrapped(iterate, 1), forcing, weight_nb, diagonal)
    residue = coarsen(defect(wrapped(iterate, 1), forcing, weight_nb, diagonal))
    if grid_level + 1 == LEVELS - 1:
        correction = coarse_solve(residue, shift_value, 0.25 ** (grid_level + 1))
    else:
        correction = vcycle_whole(grid_level + 1, None, residue, shift_value)
    iterate = iterate + refine(wrapped(correction, 1), LINEAR_EVEN, LINEAR_ODD)
    return relaxed(wrapped(iterate, 1), forcing, weight_nb, diagonal)


def collect(block):
    axes = ("gx", "gy", "gz")
    counts = [lax.axis_size(axis) for axis in axes]
    copies = jnp.broadcast_to(block[None], (math.prod(counts),) + block.shape)
    gathered = lax.all_to_all(copies, axes, 0, 0)
    extent_first, extent_second, extent_third = block.shape
    gathered = gathered.reshape(counts + list(block.shape))
    gathered = jnp.transpose(gathered, (0, 3, 2, 4, 1, 5))
    return gathered.reshape(
        counts[0] * extent_first, counts[2] * extent_second, counts[1] * extent_third
    )


def own_block(whole, width, block_shape):
    padded = jnp.pad(whole, width, mode="wrap")
    starts = (
        lax.axis_index("gx") * block_shape[0],
        lax.axis_index("gz") * block_shape[1],
        lax.axis_index("gy") * block_shape[2],
    )
    extents = (block_shape[0] + 2 * width, block_shape[1] + 2 * width, block_shape[2] + 2 * width)
    return lax.dynamic_slice(padded, starts, extents)


def face_halo(block):
    corners = jnp.pad(block, 1)
    for axis, dim in (("gx", 0), ("gy", 2), ("gz", 1)):
        count = lax.axis_size(axis)
        forward = [(i, (i + 1) % count) for i in range(count)]
        backward = [(target, source) for source, target in forward]
        extent = block.shape[dim]
        low = lax.ppermute(
            lax.slice_in_dim(block, extent - 1, None, axis=dim), axis, forward
        )
        high = lax.ppermute(lax.slice_in_dim(block, 0, 1, axis=dim), axis, backward)
        starts = [1, 1, 1]
        starts[dim] = 0
        corners = lax.dynamic_update_slice(corners, low, starts)
        starts[dim] = extent + 1
        corners = lax.dynamic_update_slice(corners, high, starts)
    return corners


def per_device_plain(source, shift):
    shift_value = shift[0]
    source_rim = face_halo(source)
    own_coarse = coarsen(source)
    sources = [None, collect(own_coarse)]
    for grid_level in range(2, LEVELS):
        sources.append(coarsen(sources[-1]))
    whole = coarse_solve(sources[-1], shift_value, 0.25 ** (LEVELS - 1))
    for grid_level in range(LEVELS - 2, 0, -1):
        whole = refine(wrapped(whole, 2), CUBIC_EVEN, CUBIC_ODD)
        whole = vcycle_whole(grid_level, whole, sources[grid_level], shift_value)
    diagonal = 6.0 + shift_value
    iterate = refine(own_block(whole, 3, own_coarse.shape), CUBIC_EVEN, CUBIC_ODD)
    iterate = relaxed(iterate, source_rim, 1.0, diagonal)
    residue = coarsen(defect(iterate, source, 1.0, diagonal))
    correction = vcycle_whole(1, None, collect(residue), shift_value)
    rim = refine(own_block(correction, 2, own_coarse.shape), LINEAR_EVEN, LINEAR_ODD)
    iterate = iterate + rim[1:-1, 1:-1, 1:-1]
    return relaxed(iterate, source, 1.0, diagonal)


def halving(count):
    matrix = np.zeros((count // 2, count))
    for cell in range(count):
        matrix[cell // 2, cell] = 1.0
    return matrix


def doubling(cells, count, even_weights, odd_weights, start=0, periodic=True):
    matrix = np.zeros((len(cells), count))
    margin = len(even_weights) // 2
    for row, cell in enumerate(cells):
        if cell is None:
            continue
        weights = odd_weights if cell % 2 else even_weights
        first = cell // 2 - margin + cell % 2
        for offset, weight in enumerate(weights):
            column = first + offset - start
            matrix[row, column % count if periodic else column] += weight
    return matrix


def pieces(matrix):
    rest = np.asarray(matrix, np.float64)
    found = []
    while np.any(rest) and len(found) < 3:
        part = rest.astype(jnp.bfloat16)
        found.append(part)
        rest = rest - part.astype(np.float64)
    return found


def ring_cells(extent, total, margin):
    cells = [None] * total
    for cell in range(-margin, extent + margin):
        cells[cell % total] = cell
    return cells


def split_values(values):
    high = values.astype(jnp.bfloat16)
    rest = values - high.astype(jnp.float32)
    middle = rest.astype(jnp.bfloat16)
    low = (rest - middle.astype(jnp.float32)).astype(jnp.bfloat16)
    return (low, middle, high)


def from_left(matrix_refs, values):
    total = None
    parts = split_values(values)
    for piece in reversed(range(len(matrix_refs))):
        for part in parts[piece:]:
            term = jnp.dot(matrix_refs[piece][...], part, preferred_element_type=jnp.float32)
            total = term if total is None else total + term
    return total


def from_right(values, matrix_refs):
    total = None
    parts = split_values(values)
    for piece in reversed(range(len(matrix_refs))):
        for part in parts[piece:]:
            term = jnp.dot(part, matrix_refs[piece][...], preferred_element_type=jnp.float32)
            total = term if total is None else total + term
    return total


def flat(values):
    return values.reshape(values.shape[0] * values.shape[1], values.shape[2])


def beside_rolled(values, periodic_first):
    if periodic_first:
        total = jnp.concatenate([values[1:], values[:1]], axis=0) + jnp.concatenate(
            [values[-1:], values[:-1]], axis=0
        )
        center = values
    else:
        total = values[2:] + values[:-2]
        center = values[1:-1]
    for axis in (1, 2):
        extent = values.shape[axis]
        total = total + (pltpu.roll(center, 1, axis) + pltpu.roll(center, extent - 1, axis))
    return (center, total)


def defect_rolled(values, forcing, weight_nb, diagonal, periodic_first=True):
    center, total = beside_rolled(values, periodic_first)
    return forcing - (diagonal * center - weight_nb * total)


def damping_over(diagonal, extent):
    return jnp.full((1, 1, extent), DAMPING, jnp.float32) / diagonal


def sweep_rolled(values, forcing, weight_nb, diagonal, periodic_first=True):
    center, total = beside_rolled(values, periodic_first)
    scale = damping_over(diagonal, values.shape[2])
    return center + scale * (forcing - (diagonal * center - weight_nb * total))


def level_tables(grid_level, shape):
    first, second, third = shape
    found = {}
    found["rows_down"] = pieces(np.kron(halving(first), halving(second)))
    found["lanes_down"] = pieces(0.125 * halving(third).T)
    for name, even, odd in (
        ("linear", LINEAR_EVEN, LINEAR_ODD),
        ("cubic", CUBIC_EVEN, CUBIC_ODD),
    ):
        up = [doubling(range(count), count // 2, even, odd) for count in shape]
        found["rows_" + name] = pieces(np.kron(up[0], up[1]))
        found["lanes_" + name] = pieces(up[2].T)
    return {(grid_level, name): value for name, value in found.items()}


def kept_products(length):
    return [(piece, part) for piece in range(length) for part in range(3 - piece)]


def joined(matrix, axis):
    found = pieces(matrix)
    order = [found[piece] for piece, _ in kept_products(len(found))]
    return [np.concatenate(order, axis=axis)]


def join_values(values, length, axis):
    parts = split_values(values)[::-1]
    chosen = [parts[part] for _, part in kept_products(length)]
    return jnp.concatenate(chosen, axis=axis)


def pieces_joined(joined_extent, extent):
    for length in (1, 2, 3):
        if len(kept_products(length)) * extent == joined_extent:
            return length
    raise ValueError("table extent")


def joined_left(table_ref, values):
    length = pieces_joined(table_ref.shape[1], values.shape[0])
    return jnp.dot(
        table_ref[...], join_values(values, length, 0), preferred_element_type=jnp.float32
    )


def joined_right(values, table_ref):
    length = pieces_joined(table_ref.shape[0], values.shape[1])
    return jnp.dot(
        join_values(values, length, 1), table_ref[...], preferred_element_type=jnp.float32
    )


def solve_tables(fine_shape):
    shape = tuple(count // 2 for count in fine_shape)

    def hartley(count):
        indices = np.arange(count)
        angles = 2.0 * np.pi * (indices[:, None] * indices[None, :] % count) / count
        return np.cos(angles) + np.sin(angles)

    cosines = [np.cos(2.0 * np.pi * np.arange(count) / count) for count in shape]
    spread = (
        6.0
        - 2.0 * cosines[0][:, None, None]
        - 2.0 * cosines[1][None, :, None]
        - 2.0 * cosines[2][None, None, :]
    )
    spread = 0.25 ** (LEVELS - 1) * spread.reshape(shape[0] * shape[1], shape[2])
    padding = -shape[2] % 128
    spread = np.pad(spread, ((0, 0), (0, padding)), constant_values=1.0)
    to_modes = [hartley(coarse) @ halving(fine) for coarse, fine in zip(shape, fine_shape)]
    found = {
        ("solve", "rows_to"): joined(np.kron(to_modes[0], to_modes[1]), 1),
        ("solve", "lanes_to"): joined(np.pad(0.125 * to_modes[2].T, ((0, 0), (0, padding))), 0),
        ("solve", "spread"): [spread.astype(np.float32)],
    }
    for name, even, odd in (
        ("linear", LINEAR_EVEN, LINEAR_ODD),
        ("cubic", CUBIC_EVEN, CUBIC_ODD),
    ):
        back = [
            doubling(range(fine), coarse, even, odd) @ hartley(coarse) / coarse
            for coarse, fine in zip(shape, fine_shape)
        ]
        found["solve", "rows_" + name] = joined(np.kron(back[0], back[1]), 1)
        found["solve", "lanes_" + name] = joined(np.pad(back[2].T, ((0, padding), (0, 0))), 0)
    return found


def solve_up(tables_of, name, forcing, shift_value):
    modes = joined_left(tables_of["solve", "rows_to"][0], flat(forcing))
    modes = joined_right(modes, tables_of["solve", "lanes_to"][0])
    modes = modes / (tables_of["solve", "spread"][0][...] + shift_value)
    wide = joined_right(modes, tables_of["solve", "lanes_" + name][0])
    wide = joined_left(tables_of["solve", "rows_" + name][0], wide)
    return wide.reshape(forcing.shape)


def down(tables_of, grid_level, values):
    coarse = from_left(tables_of[grid_level, "rows_down"], flat(values))
    return from_right(coarse, tables_of[grid_level, "lanes_down"])


def up(tables_of, grid_level, name, values, shape):
    wide = from_right(values, tables_of[grid_level, "lanes_" + name])
    return from_left(tables_of[grid_level, "rows_" + name], wide).reshape(shape)


def vcycle_rolled(tables_of, grid_level, iterate, forcing, shift_value):
    weight_nb = 0.25**grid_level
    diagonal = 6.0 * weight_nb + shift_value
    shape = forcing.shape
    if iterate is None:
        iterate = damping_over(diagonal, shape[2]) * forcing
    else:
        iterate = sweep_rolled(iterate, forcing, weight_nb, diagonal)
    residue = defect_rolled(iterate, forcing, weight_nb, diagonal)
    if grid_level + 1 == LEVELS - 1:
        iterate = iterate + solve_up(tables_of, "linear", residue, shift_value)
    else:
        residue = down(tables_of, grid_level, residue)
        coarse_shape = tuple(extent // 2 for extent in shape)
        correction = flat(
            vcycle_rolled(
                tables_of, grid_level + 1, None, residue.reshape(coarse_shape), shift_value
            )
        )
        iterate = iterate + up(tables_of, grid_level, "linear", correction, shape)
    return sweep_rolled(iterate, forcing, weight_nb, diagonal)


def pack(tables_of, values):
    coarse = from_left(tables_of["own", "rows_down"], flat(values))
    half = coarse.shape[0] // 2
    return from_right(coarse[:half], tables_of["own", "left_down"]) + from_right(
        coarse[half:], tables_of["own", "right_down"]
    )


def unpack(gathered_ref, whole_ref, counts, extents):
    half, second, lanes = (extents[0] // 2, extents[1], 2 * extents[2])
    low_lane = lax.broadcasted_iota(jnp.int32, (half, second, lanes), 2) < extents[2]
    for x in range(counts[0]):
        for z in range(counts[2]):
            for pair in range(counts[1] // 2):
                blocks = [
                    gathered_ref[(x * counts[1] + 2 * pair + side) * counts[2] + z].reshape(
                        half, second, lanes
                    )
                    for side in range(2)
                ]
                turned = [pltpu.roll(block, extents[2], 2) for block in blocks]
                window = (pl.ds(z * second, second), pl.ds(pair * lanes, lanes))
                whole_ref[(pl.ds(x * 2 * half, half), *window)] = jnp.where(
                    low_lane, blocks[0], turned[1]
                )
                whole_ref[(pl.ds(x * 2 * half + half, half), *window)] = jnp.where(
                    low_lane, turned[0], blocks[1]
                )


def own_window(whole, scratch_ref, margin, extents, place_ref):
    count = whole.shape[0]
    scratch_ref[pl.ds(margin, count)] = whole
    scratch_ref[pl.ds(0, margin)] = whole[count - margin :]
    scratch_ref[pl.ds(margin + count, margin)] = whole[:margin]
    cut = scratch_ref[pl.ds(place_ref[0] * extents[0], extents[0] + 2 * margin)]
    turn_second = (whole.shape[1] - place_ref[1] * extents[1]) % whole.shape[1]
    turn_third = (whole.shape[2] - place_ref[2] * extents[2]) % whole.shape[2]
    return pltpu.roll(pltpu.roll(cut, turn_second, 1), turn_third, 2)


def with_tables(body, tables_map, n_plain):
    keys = [(key, len(value)) for key, value in tables_map.items()]
    arrays = [jnp.asarray(part) for value in tables_map.values() for part in value]

    def kernel(*refs):
        position = n_plain
        tables_of = {}
        for key, length in keys:
            tables_of[key] = refs[position : position + length]
            position += length
        body(tables_of, refs[:n_plain], refs[position:])

    return (kernel, arrays)


def per_device_kernels(source, shift):
    counts = tuple(lax.axis_size(axis) for axis in ("gx", "gy", "gz"))
    block = source.shape
    extents = tuple(extent // 2 for extent in block)
    shape = (extents[0] * counts[0], extents[1] * counts[2], extents[2] * counts[1])
    place = jnp.stack([lax.axis_index("gx"), lax.axis_index("gz"), lax.axis_index("gy")])
    devices = math.prod(counts)
    rows_wide = block[1] + 8
    lanes_wide = 2 * block[2]
    vmem = pl.BlockSpec(memory_space=pltpu.VMEM)
    smem = pl.BlockSpec(memory_space=pltpu.SMEM)

    own = {("own", "rows_down"): pieces(np.kron(halving(block[0]), halving(block[1])))}
    narrow = 0.125 * halving(block[2]).T
    own["own", "left_down"] = pieces(np.concatenate([narrow, 0.0 * narrow], axis=1))
    own["own", "right_down"] = pieces(np.concatenate([0.0 * narrow, narrow], axis=1))

    def edge_tables(name, even, odd, margin):
        fine = margin
        coarse = len(even) // 2 + 1
        first = doubling(
            range(-fine, block[0] + fine), extents[0] + 2 * coarse, even, odd, -coarse, False
        )
        second = doubling(ring_cells(block[1], rows_wide, fine), shape[1], even, odd)
        third = doubling(ring_cells(block[2], lanes_wide, fine), shape[2], even, odd)
        return {
            ("own", "rows_" + name): pieces(np.kron(first, second)),
            ("own", "lanes_" + name): pieces(third.T),
        }

    levels = {}
    for grid_level in range(1, LEVELS - 2):
        levels.update(
            level_tables(grid_level, tuple(extent >> (grid_level - 1) for extent in shape))
        )
    levels.update(solve_tables(tuple(extent >> (LEVELS - 3) for extent in shape)))

    def gather(copies):
        return lax.all_to_all(copies, ("gx", "gy", "gz"), 0, 0)

    copies_shape = jax.ShapeDtypeStruct(
        (devices, extents[0] // 2 * extents[1], 2 * extents[2]), jnp.float32
    )

    def pack_body(tables_of, ins, outs):
        values = ins[0][...]
        outs[0][...] = jnp.broadcast_to(pack(tables_of, values)[None], copies_shape.shape)
        lane = lax.broadcasted_iota(jnp.int32, block, 2)
        square = (block[0], block[1], block[1])
        same = lax.broadcasted_iota(jnp.int32, square, 1) == lax.broadcasted_iota(
            jnp.int32, square, 2
        )
        for out_ref, chosen in ((outs[1], block[2] - 1), (outs[2], 0)):
            face = jnp.sum(jnp.where(lane == chosen, values, 0.0), axis=2, keepdims=True)
            face = jnp.where(same, jnp.broadcast_to(face, square), 0.0)
            out_ref[...] = jnp.sum(face, axis=1, keepdims=True)

    kernel, arrays = with_tables(pack_body, own, 1)
    face_shape = jax.ShapeDtypeStruct((block[0], 1, block[1]), jnp.float32)
    copies, last_third, first_third = pl.pallas_call(
        kernel,
        out_shape=(copies_shape, face_shape, face_shape),
        in_specs=[vmem] * (1 + len(arrays)),
        out_specs=(vmem, vmem, vmem),
        name="pack",
    )(source, *arrays)

    def ring_shift(values, axis, step):
        count = lax.axis_size(axis)
        return lax.ppermute(values, axis, [(i, (i + step) % count) for i in range(count)])

    rims = [
        ring_shift(source[block[0] - 1 :], "gx", 1),
        ring_shift(source[:1], "gx", -1),
    ]
    last_second = source[:, block[1] - 1 :]
    first_second = source[:, :1]
    if counts[2] == 2:
        rims.append(ring_shift(jnp.stack([last_second, first_second]), "gz", 1))
    else:
        rims.append(
            jnp.stack([ring_shift(last_second, "gz", 1), ring_shift(first_second, "gz", -1)])
        )
    rims.append(ring_shift(last_third, "gy", 1))
    rims.append(ring_shift(first_third, "gy", -1))
    gathered = gather(copies)

    def first_body(tables_of, ins, outs):
        shift_ref, place_ref, gathered_ref, source_ref = ins[:4]
        low_first, high_first, both_second, low_third, high_third = ins[4:]
        copies_ref, iterate_ref, whole_ref, scratch_ref = outs
        shift_value = shift_ref[0]
        unpack(gathered_ref, whole_ref, counts, extents)
        whole_forcing = whole_ref[...]
        forcings = [whole_forcing]
        for grid_level in range(1, LEVELS - 2):
            fine = forcings[-1]
            coarse = down(tables_of, grid_level, fine)
            forcings.append(coarse.reshape(tuple(extent // 2 for extent in fine.shape)))
        iterate = solve_up(tables_of, "cubic", forcings[-1], shift_value)
        for grid_level in range(LEVELS - 2, 0, -1):
            forcing = forcings[grid_level - 1]
            if grid_level < LEVELS - 2:
                iterate = up(tables_of, grid_level, "cubic", flat(iterate), forcing.shape)
            iterate = vcycle_rolled(tables_of, grid_level, iterate, forcing, shift_value)
        window = own_window(iterate, scratch_ref, 3, extents, place_ref)
        iterate = from_right(flat(window), tables_of["own", "lanes_cubic"])
        iterate = from_left(tables_of["own", "rows_cubic"], iterate)
        iterate = iterate.reshape(block[0] + 4, rows_wide, lanes_wide)

        wide = (block[0], rows_wide, lanes_wide)
        row = lax.broadcasted_iota(jnp.int32, wide, 1)
        lane = lax.broadcasted_iota(jnp.int32, wide, 2)

        def widened(values):
            first = values.shape[0]
            values = jnp.concatenate([values, jnp.zeros_like(values[:, :8])], axis=1)
            return jnp.concatenate([values, jnp.zeros((first, rows_wide, block[2]))], axis=2)

        def rows_only(values):
            values = jnp.concatenate([values, jnp.zeros_like(values)], axis=2)
            return jnp.broadcast_to(values, wide)

        def lanes_only(values):
            square = (block[0], block[1], block[1])
            same = lax.broadcasted_iota(jnp.int32, square, 1) == lax.broadcasted_iota(
                jnp.int32, square, 2
            )
            values = jnp.where(same, jnp.broadcast_to(values, square), 0.0)
            values = jnp.sum(values, axis=2, keepdims=True)
            values = jnp.broadcast_to(values, (block[0], block[1], lanes_wide))
            return jnp.concatenate([values, jnp.zeros_like(values[:, :8])], axis=1)

        middle = widened(source_ref[...])
        middle = jnp.where(row == block[1], rows_only(both_second[1]), middle)
        middle = jnp.where(row == rows_wide - 1, rows_only(both_second[0]), middle)
        middle = jnp.where(lane == block[2], lanes_only(high_third[...]), middle)
        middle = jnp.where(lane == lanes_wide - 1, lanes_only(low_third[...]), middle)
        forcing = jnp.concatenate(
            [widened(low_first[...]), middle, widened(high_first[...])], axis=0
        )
        diagonal = 6.0 + shift_value
        iterate = sweep_rolled(iterate, forcing, 1.0, diagonal, False)
        iterate_ref[...] = iterate
        residue = defect_rolled(iterate, middle, 1.0, diagonal, False)
        packed = pack(tables_of, residue[:, : block[1], : block[2]])
        copies_ref[...] = jnp.broadcast_to(packed[None], copies_ref.shape)

    tables_map = {**levels, **own, **edge_tables("cubic", CUBIC_EVEN, CUBIC_ODD, 2)}
    kernel, arrays = with_tables(first_body, tables_map, 9)
    iterate_shape = jax.ShapeDtypeStruct((block[0] + 2, rows_wide, lanes_wide), jnp.float32)
    copies, iterate = pl.pallas_call(
        kernel,
        out_shape=(copies_shape, iterate_shape),
        in_specs=[smem, smem] + [vmem] * (7 + len(arrays)),
        out_specs=(vmem, vmem),
        scratch_shapes=[
            pltpu.VMEM(shape, jnp.float32),
            pltpu.VMEM((shape[0] + 6, *shape[1:]), jnp.float32),
        ],
        name="first",
    )(shift, place, gathered, source, *rims, *arrays)
    gathered = gather(copies)

    def second_body(tables_of, ins, outs):
        shift_ref, place_ref, gathered_ref, source_ref, iterate_ref = ins
        result_ref, whole_ref, scratch_ref = outs
        shift_value = shift_ref[0]
        unpack(gathered_ref, whole_ref, counts, extents)
        correction = vcycle_rolled(tables_of, 1, None, whole_ref[...], shift_value)
        window = own_window(correction, scratch_ref, 2, extents, place_ref)
        wide = from_right(flat(window), tables_of["own", "lanes_linear"])
        wide = from_left(tables_of["own", "rows_linear"], wide).reshape(iterate_shape.shape)
        iterate = iterate_ref[...] + wide
        center, total = beside_rolled(iterate, False)
        center = center[:, : block[1], : block[2]]
        total = total[:, : block[1], : block[2]]
        diagonal = 6.0 + shift_value
        scale = damping_over(diagonal, block[2])
        result_ref[...] = center + scale * (source_ref[...] - (diagonal * center - total))

    tables_map = {key: value for key, value in levels.items() if "cubic" not in key[1]}
    tables_map.update(edge_tables("linear", LINEAR_EVEN, LINEAR_ODD, 1))
    kernel, arrays = with_tables(second_body, tables_map, 5)
    return pl.pallas_call(
        kernel,
        out_shape=jax.ShapeDtypeStruct(block, jnp.float32),
        in_specs=[smem, smem] + [vmem] * (3 + len(arrays)),
        out_specs=vmem,
        scratch_shapes=[
            pltpu.VMEM(shape, jnp.float32),
            pltpu.VMEM((shape[0] + 4, *shape[1:]), jnp.float32),
        ],
        name="second",
    )(shift, place, gathered, source, iterate, *arrays)


WHOLE_LIMIT = 1 << 18


def per_device(source, shift):
    block = source.shape
    counts = tuple(lax.axis_size(axis) for axis in ("gx", "gy", "gz"))
    cells = math.prod(block) // 8 * math.prod(counts)
    second_deep = block[1] * counts[2] >> (LEVELS - 2)
    third_deep = block[2] * counts[1] >> (LEVELS - 2)
    aligned = (
        block[0] % 4 == 0
        and block[1] % 16 == 0
        and block[2] == 128
        and counts[1] % 2 == 0
        and second_deep % 8 == 0
        and third_deep % 128 == 0
        and block[0] * counts[0] >= 32
    )
    if aligned and cells <= WHOLE_LIMIT:
        return per_device_kernels(source, shift)
    return per_device_plain(source, shift)


def solution(mesh):
    in_specs = (P("gx", "gz", "gy"), P())
    out_specs = P("gx", "gz", "gy")
    return jax.shard_map(
        per_device, mesh=mesh, in_specs=in_specs, out_specs=out_specs, check_vma=False
    )
```

```python
import math

import jax
import jax.numpy as jnp
import numpy as np
from jax import lax
from jax.experimental import pallas as pl
from jax.experimental.pallas import tpu as pltpu
from jax.sharding import PartitionSpec as P

LEVELS = 4


DAMPING = 6.0 / 7.0
PRECISE = lax.Precision.HIGHEST
CUBIC_EVEN = (-5.0 / 128.0, 35.0 / 128.0, 105.0 / 128.0, -7.0 / 128.0)
CUBIC_ODD = (-7.0 / 128.0, 105.0 / 128.0, 35.0 / 128.0, -5.0 / 128.0)
LINEAR_EVEN = (0.25, 0.75)
LINEAR_ODD = (0.75, 0.25)


def extended(block, sides, width):
    for axis, dim in sides:
        count = lax.axis_size(axis)
        forward = [(i, i + 1) for i in range(count - 1)]
        forward.append((count - 1, 0))
        backward = [(target, source) for source, target in forward]
        low = lax.ppermute(
            lax.slice_in_dim(block, block.shape[dim] - width, None, axis=dim), axis, forward
        )
        high = lax.ppermute(lax.slice_in_dim(block, 0, width, axis=dim), axis, backward)
        block = jnp.concatenate([low, block, high], axis=dim)
    return block


def wrapped(values, width):
    return jnp.pad(values, width, mode="wrap")


def neighbours(padded):
    center = padded[1:-1, 1:-1, 1:-1]
    beside_all = padded[2:, 1:-1, 1:-1] + padded[:-2, 1:-1, 1:-1]
    beside_all = beside_all + padded[1:-1, 2:, 1:-1] + padded[1:-1, :-2, 1:-1]
    beside_all = beside_all + padded[1:-1, 1:-1, 2:] + padded[1:-1, 1:-1, :-2]
    return (center, beside_all)


def defect(padded, forcing, weight_nb, diagonal):
    center, beside_all = neighbours(padded)
    return forcing - (diagonal * center - weight_nb * beside_all)


def relaxed(padded, forcing, weight_nb, diagonal):
    center, beside_all = neighbours(padded)
    return center + DAMPING * (forcing - (diagonal * center - weight_nb * beside_all)) / diagonal


def coarsen(values):
    values = values[0::2] + values[1::2]
    values = values[:, 0::2] + values[:, 1::2]
    values = values[:, :, 0::2] + values[:, :, 1::2]
    return 0.125 * values


def refine_axis(padded, dimension, even_weights, odd_weights):
    margin = len(even_weights) // 2
    length = padded.shape[dimension] - 2 * margin
    even_cells = even_weights[0] * lax.slice_in_dim(padded, 0, length, axis=dimension)
    odd_cells = odd_weights[0] * lax.slice_in_dim(padded, 1, 1 + length, axis=dimension)
    for offset in range(1, len(even_weights)):
        even_cells = even_cells + even_weights[offset] * lax.slice_in_dim(
            padded, offset, offset + length, axis=dimension
        )
        odd_cells = odd_cells + odd_weights[offset] * lax.slice_in_dim(
            padded, offset + 1, offset + 1 + length, axis=dimension
        )
    stacked = jnp.stack([even_cells, odd_cells], axis=dimension + 1)
    new_shape = list(even_cells.shape)
    new_shape[dimension] = 2 * length
    return stacked.reshape(new_shape)


def refine(padded, even_weights, odd_weights):
    for dimension in range(3):
        padded = refine_axis(padded, dimension, even_weights, odd_weights)
    return padded


def tables(cells_count):
    indices = jnp.arange(cells_count, dtype=jnp.int32)
    angles = (indices[:, None] * indices[None, :] % cells_count).astype(jnp.float32) * (
        2.0 * math.pi / cells_count
    )
    return (jnp.cos(angles), jnp.sin(angles))


def along_axis(matrix, values, dimension):
    product = jnp.tensordot(matrix, values, axes=([1], [dimension]), precision=PRECISE)
    return jnp.moveaxis(product, 0, dimension)


def coarse_solve(forcing, shift_value, weight_nb):
    cosine_table, sine_table = tables(forcing.shape[0])
    real_part = along_axis(cosine_table, forcing, 0)
    imag_part = -along_axis(sine_table, forcing, 0)
    for dimension in (1, 2):
        cosine_table, sine_table = tables(forcing.shape[dimension])
        real_next = along_axis(cosine_table, real_part, dimension) + along_axis(
            sine_table, imag_part, dimension
        )
        imag_part = along_axis(cosine_table, imag_part, dimension) - along_axis(
            sine_table, real_part, dimension
        )
        real_part = real_next
    cosines = [
        jnp.cos(jnp.arange(cells_count, dtype=jnp.float32) * (2.0 * math.pi / cells_count))
        for cells_count in forcing.shape
    ]
    eigenvalue = (
        weight_nb
        * (
            6.0
            - 2.0 * cosines[0][:, None, None]
            - 2.0 * cosines[1][None, :, None]
            - 2.0 * cosines[2][None, None, :]
        )
        + shift_value
    )
    real_part = real_part / eigenvalue
    imag_part = imag_part / eigenvalue
    for dimension in (0, 1):
        cosine_table, sine_table = tables(forcing.shape[dimension])
        real_next = along_axis(cosine_table, real_part, dimension) - along_axis(
            sine_table, imag_part, dimension
        )
        imag_part = along_axis(cosine_table, imag_part, dimension) + along_axis(
            sine_table, real_part, dimension
        )
        real_part = real_next
    cosine_table, sine_table = tables(forcing.shape[2])
    real_part = along_axis(cosine_table, real_part, 2) - along_axis(sine_table, imag_part, 2)
    return real_part / float(forcing.size)


def vcycle_whole(grid_level, iterate, forcing, shift_value):
    weight_nb = 0.25**grid_level
    diagonal = 6.0 * weight_nb + shift_value
    if iterate is None:
        iterate = DAMPING * forcing / diagonal
    else:
        iterate = relaxed(wrapped(iterate, 1), forcing, weight_nb, diagonal)
    residue = coarsen(defect(wrapped(iterate, 1), forcing, weight_nb, diagonal))
    if grid_level + 1 == LEVELS - 1:
        correction = coarse_solve(residue, shift_value, 0.25 ** (grid_level + 1))
    else:
        correction = vcycle_whole(grid_level + 1, None, residue, shift_value)
    iterate = iterate + refine(wrapped(correction, 1), LINEAR_EVEN, LINEAR_ODD)
    return relaxed(wrapped(iterate, 1), forcing, weight_nb, diagonal)


def collect(block):
    axes = ("gx", "gy", "gz")
    counts = [lax.axis_size(axis) for axis in axes]
    copies = jnp.broadcast_to(block[None], (math.prod(counts),) + block.shape)
    gathered = lax.all_to_all(copies, axes, 0, 0)
    extent_first, extent_second, extent_third = block.shape
    gathered = gathered.reshape(counts + list(block.shape))
    gathered = jnp.transpose(gathered, (0, 3, 2, 4, 1, 5))
    return gathered.reshape(
        counts[0] * extent_first, counts[2] * extent_second, counts[1] * extent_third
    )


def own_block(whole, width, block_shape):
    padded = jnp.pad(whole, width, mode="wrap")
    starts = (
        lax.axis_index("gx") * block_shape[0],
        lax.axis_index("gz") * block_shape[1],
        lax.axis_index("gy") * block_shape[2],
    )
    extents = (block_shape[0] + 2 * width, block_shape[1] + 2 * width, block_shape[2] + 2 * width)
    return lax.dynamic_slice(padded, starts, extents)


def face_halo(block):
    corners = jnp.pad(block, 1)
    for axis, dim in (("gx", 0), ("gy", 2), ("gz", 1)):
        count = lax.axis_size(axis)
        forward = [(i, (i + 1) % count) for i in range(count)]
        backward = [(target, source) for source, target in forward]
        extent = block.shape[dim]
        low = lax.ppermute(
            lax.slice_in_dim(block, extent - 1, None, axis=dim), axis, forward
        )
        high = lax.ppermute(lax.slice_in_dim(block, 0, 1, axis=dim), axis, backward)
        starts = [1, 1, 1]
        starts[dim] = 0
        corners = lax.dynamic_update_slice(corners, low, starts)
        starts[dim] = extent + 1
        corners = lax.dynamic_update_slice(corners, high, starts)
    return corners


def per_device_plain(source, shift):
    shift_value = shift[0]
    source_rim = face_halo(source)
    own_coarse = coarsen(source)
    sources = [None, collect(own_coarse)]
    for grid_level in range(2, LEVELS):
        sources.append(coarsen(sources[-1]))
    whole = coarse_solve(sources[-1], shift_value, 0.25 ** (LEVELS - 1))
    for grid_level in range(LEVELS - 2, 0, -1):
        whole = refine(wrapped(whole, 2), CUBIC_EVEN, CUBIC_ODD)
        whole = vcycle_whole(grid_level, whole, sources[grid_level], shift_value)
    diagonal = 6.0 + shift_value
    iterate = refine(own_block(whole, 3, own_coarse.shape), CUBIC_EVEN, CUBIC_ODD)
    iterate = relaxed(iterate, source_rim, 1.0, diagonal)
    residue = coarsen(defect(iterate, source, 1.0, diagonal))
    correction = vcycle_whole(1, None, collect(residue), shift_value)
    rim = refine(own_block(correction, 2, own_coarse.shape), LINEAR_EVEN, LINEAR_ODD)
    iterate = iterate + rim[1:-1, 1:-1, 1:-1]
    return relaxed(iterate, source, 1.0, diagonal)


def halving(count):
    matrix = np.zeros((count // 2, count))
    for cell in range(count):
        matrix[cell // 2, cell] = 1.0
    return matrix


def doubling(cells, count, even_weights, odd_weights, start=0, periodic=True):
    matrix = np.zeros((len(cells), count))
    margin = len(even_weights) // 2
    for row, cell in enumerate(cells):
        if cell is None:
            continue
        weights = odd_weights if cell % 2 else even_weights
        first = cell // 2 - margin + cell % 2
        for offset, weight in enumerate(weights):
            column = first + offset - start
            matrix[row, column % count if periodic else column] += weight
    return matrix


def pieces(matrix):
    rest = np.asarray(matrix, np.float64)
    found = []
    while np.any(rest) and len(found) < 3:
        part = rest.astype(jnp.bfloat16)
        found.append(part)
        rest = rest - part.astype(np.float64)
    return found


def ring_cells(extent, total, margin):
    cells = [None] * total
    for cell in range(-margin, extent + margin):
        cells[cell % total] = cell
    return cells


def split_values(values):
    high = values.astype(jnp.bfloat16)
    rest = values - high.astype(jnp.float32)
    middle = rest.astype(jnp.bfloat16)
    low = (rest - middle.astype(jnp.float32)).astype(jnp.bfloat16)
    return (low, middle, high)


def from_left(matrix_refs, values):
    total = None
    parts = split_values(values)
    for piece in reversed(range(len(matrix_refs))):
        for part in parts[piece:]:
            term = jnp.dot(matrix_refs[piece][...], part, preferred_element_type=jnp.float32)
            total = term if total is None else total + term
    return total


def from_right(values, matrix_refs):
    total = None
    parts = split_values(values)
    for piece in reversed(range(len(matrix_refs))):
        for part in parts[piece:]:
            term = jnp.dot(part, matrix_refs[piece][...], preferred_element_type=jnp.float32)
            total = term if total is None else total + term
    return total


def flat(values):
    return values.reshape(values.shape[0] * values.shape[1], values.shape[2])


def beside_rolled(values, periodic_first):
    if periodic_first:
        total = jnp.concatenate([values[1:], values[:1]], axis=0) + jnp.concatenate(
            [values[-1:], values[:-1]], axis=0
        )
        center = values
    else:
        total = values[2:] + values[:-2]
        center = values[1:-1]
    for axis in (1, 2):
        extent = values.shape[axis]
        total = total + (pltpu.roll(center, 1, axis) + pltpu.roll(center, extent - 1, axis))
    return (center, total)


def defect_rolled(values, forcing, weight_nb, diagonal, periodic_first=True):
    center, total = beside_rolled(values, periodic_first)
    return forcing - (diagonal * center - weight_nb * total)


def damping_over(diagonal, extent):
    return jnp.full((1, 1, extent), DAMPING, jnp.float32) / diagonal


def sweep_rolled(values, forcing, weight_nb, diagonal, periodic_first=True):
    center, total = beside_rolled(values, periodic_first)
    scale = damping_over(diagonal, values.shape[2])
    return center + scale * (forcing - (diagonal * center - weight_nb * total))


def level_tables(grid_level, shape):
    first, second, third = shape
    found = {}
    found["rows_down"] = pieces(np.kron(halving(first), halving(second)))
    found["lanes_down"] = pieces(0.125 * halving(third).T)
    for name, even, odd in (
        ("linear", LINEAR_EVEN, LINEAR_ODD),
        ("cubic", CUBIC_EVEN, CUBIC_ODD),
    ):
        up = [doubling(range(count), count // 2, even, odd) for count in shape]
        found["rows_" + name] = pieces(np.kron(up[0], up[1]))
        found["lanes_" + name] = pieces(up[2].T)
    return {(grid_level, name): value for name, value in found.items()}


def kept_products(length):
    return [(piece, part) for piece in range(length) for part in range(3 - piece)]


def joined(matrix, axis):
    found = pieces(matrix)
    order = [found[piece] for piece, _ in kept_products(len(found))]
    return [np.concatenate(order, axis=axis)]


def join_values(values, length, axis):
    parts = split_values(values)[::-1]
    chosen = [parts[part] for _, part in kept_products(length)]
    return jnp.concatenate(chosen, axis=axis)


def pieces_joined(joined_extent, extent):
    for length in (1, 2, 3):
        if len(kept_products(length)) * extent == joined_extent:
            return length
    raise ValueError("table extent")


def joined_left(table_ref, values):
    length = pieces_joined(table_ref.shape[1], values.shape[0])
    return jnp.dot(
        table_ref[...], join_values(values, length, 0), preferred_element_type=jnp.float32
    )


def joined_right(values, table_ref):
    length = pieces_joined(table_ref.shape[0], values.shape[1])
    return jnp.dot(
        join_values(values, length, 1), table_ref[...], preferred_element_type=jnp.float32
    )


def solve_tables(fine_shape):
    shape = tuple(count // 2 for count in fine_shape)

    def hartley(count):
        indices = np.arange(count)
        angles = 2.0 * np.pi * (indices[:, None] * indices[None, :] % count) / count
        return np.cos(angles) + np.sin(angles)

    cosines = [np.cos(2.0 * np.pi * np.arange(count) / count) for count in shape]
    spread = (
        6.0
        - 2.0 * cosines[0][:, None, None]
        - 2.0 * cosines[1][None, :, None]
        - 2.0 * cosines[2][None, None, :]
    )
    spread = 0.25 ** (LEVELS - 1) * spread.reshape(shape[0] * shape[1], shape[2])
    padding = -shape[2] % 128
    spread = np.pad(spread, ((0, 0), (0, padding)), constant_values=1.0)
    to_modes = [hartley(coarse) @ halving(fine) for coarse, fine in zip(shape, fine_shape)]
    found = {
        ("solve", "rows_to"): joined(np.kron(to_modes[0], to_modes[1]), 1),
        ("solve", "lanes_to"): joined(np.pad(0.125 * to_modes[2].T, ((0, 0), (0, padding))), 0),
        ("solve", "spread"): [spread.astype(np.float32)],
    }
    for name, even, odd in (
        ("linear", LINEAR_EVEN, LINEAR_ODD),
        ("cubic", CUBIC_EVEN, CUBIC_ODD),
    ):
        back = [
            doubling(range(fine), coarse, even, odd) @ hartley(coarse) / coarse
            for coarse, fine in zip(shape, fine_shape)
        ]
        found["solve", "rows_" + name] = joined(np.kron(back[0], back[1]), 1)
        found["solve", "lanes_" + name] = joined(np.pad(back[2].T, ((0, padding), (0, 0))), 0)
    return found


def solve_up(tables_of, name, forcing, shift_value):
    modes = joined_left(tables_of["solve", "rows_to"][0], flat(forcing))
    modes = joined_right(modes, tables_of["solve", "lanes_to"][0])
    modes = modes / (tables_of["solve", "spread"][0][...] + shift_value)
    wide = joined_right(modes, tables_of["solve", "lanes_" + name][0])
    wide = joined_left(tables_of["solve", "rows_" + name][0], wide)
    return wide.reshape(forcing.shape)


def down(tables_of, grid_level, values):
    coarse = from_left(tables_of[grid_level, "rows_down"], flat(values))
    return from_right(coarse, tables_of[grid_level, "lanes_down"])


def up(tables_of, grid_level, name, values, shape):
    wide = from_right(values, tables_of[grid_level, "lanes_" + name])
    return from_left(tables_of[grid_level, "rows_" + name], wide).reshape(shape)


def vcycle_rolled(tables_of, grid_level, iterate, forcing, shift_value):
    weight_nb = 0.25**grid_level
    diagonal = 6.0 * weight_nb + shift_value
    shape = forcing.shape
    if iterate is None:
        iterate = damping_over(diagonal, shape[2]) * forcing
    else:
        iterate = sweep_rolled(iterate, forcing, weight_nb, diagonal)
    residue = defect_rolled(iterate, forcing, weight_nb, diagonal)
    if grid_level + 1 == LEVELS - 1:
        iterate = iterate + solve_up(tables_of, "linear", residue, shift_value)
    else:
        residue = down(tables_of, grid_level, residue)
        coarse_shape = tuple(extent // 2 for extent in shape)
        correction = flat(
            vcycle_rolled(
                tables_of, grid_level + 1, None, residue.reshape(coarse_shape), shift_value
            )
        )
        iterate = iterate + up(tables_of, grid_level, "linear", correction, shape)
    return sweep_rolled(iterate, forcing, weight_nb, diagonal)


def pack(tables_of, values):
    coarse = from_left(tables_of["own", "rows_down"], flat(values))
    half = coarse.shape[0] // 2
    return from_right(coarse[:half], tables_of["own", "left_down"]) + from_right(
        coarse[half:], tables_of["own", "right_down"]
    )


def unpack(gathered_ref, whole_ref, counts, extents):
    half, second, lanes = (extents[0] // 2, extents[1], 2 * extents[2])
    low_lane = lax.broadcasted_iota(jnp.int32, (half, second, lanes), 2) < extents[2]
    for x in range(counts[0]):
        for z in range(counts[2]):
            for pair in range(counts[1] // 2):
                blocks = [
                    gathered_ref[(x * counts[1] + 2 * pair + side) * counts[2] + z].reshape(
                        half, second, lanes
                    )
                    for side in range(2)
                ]
                turned = [pltpu.roll(block, extents[2], 2) for block in blocks]
                window = (pl.ds(z * second, second), pl.ds(pair * lanes, lanes))
                whole_ref[(pl.ds(x * 2 * half, half), *window)] = jnp.where(
                    low_lane, blocks[0], turned[1]
                )
                whole_ref[(pl.ds(x * 2 * half + half, half), *window)] = jnp.where(
                    low_lane, turned[0], blocks[1]
                )


def own_window(whole, scratch_ref, margin, extents, place_ref):
    count = whole.shape[0]
    scratch_ref[pl.ds(margin, count)] = whole
    scratch_ref[pl.ds(0, margin)] = whole[count - margin :]
    scratch_ref[pl.ds(margin + count, margin)] = whole[:margin]
    cut = scratch_ref[pl.ds(place_ref[0] * extents[0], extents[0] + 2 * margin)]
    turn_second = (whole.shape[1] - place_ref[1] * extents[1]) % whole.shape[1]
    turn_third = (whole.shape[2] - place_ref[2] * extents[2]) % whole.shape[2]
    return pltpu.roll(pltpu.roll(cut, turn_second, 1), turn_third, 2)


def with_tables(body, tables_map, n_plain):
    keys = [(key, len(value)) for key, value in tables_map.items()]
    arrays = [jnp.asarray(part) for value in tables_map.values() for part in value]

    def kernel(*refs):
        position = n_plain
        tables_of = {}
        for key, length in keys:
            tables_of[key] = refs[position : position + length]
            position += length
        body(tables_of, refs[:n_plain], refs[position:])

    return (kernel, arrays)


def per_device_kernels(source, shift):
    counts = tuple(lax.axis_size(axis) for axis in ("gx", "gy", "gz"))
    block = source.shape
    extents = tuple(extent // 2 for extent in block)
    shape = (extents[0] * counts[0], extents[1] * counts[2], extents[2] * counts[1])
    place = jnp.stack([lax.axis_index("gx"), lax.axis_index("gz"), lax.axis_index("gy")])
    devices = math.prod(counts)
    rows_wide = block[1] + 8
    lanes_wide = 2 * block[2]
    vmem = pl.BlockSpec(memory_space=pltpu.VMEM)
    smem = pl.BlockSpec(memory_space=pltpu.SMEM)

    own = {("own", "rows_down"): pieces(np.kron(halving(block[0]), halving(block[1])))}
    narrow = 0.125 * halving(block[2]).T
    own["own", "left_down"] = pieces(np.concatenate([narrow, 0.0 * narrow], axis=1))
    own["own", "right_down"] = pieces(np.concatenate([0.0 * narrow, narrow], axis=1))

    def edge_tables(name, even, odd, margin):
        fine = margin
        coarse = len(even) // 2 + 1
        first = doubling(
            range(-fine, block[0] + fine), extents[0] + 2 * coarse, even, odd, -coarse, False
        )
        second = doubling(ring_cells(block[1], rows_wide, fine), shape[1], even, odd)
        third = doubling(ring_cells(block[2], lanes_wide, fine), shape[2], even, odd)
        return {
            ("own", "rows_" + name): pieces(np.kron(first, second)),
            ("own", "lanes_" + name): pieces(third.T),
        }

    levels = {}
    for grid_level in range(1, LEVELS - 2):
        levels.update(
            level_tables(grid_level, tuple(extent >> (grid_level - 1) for extent in shape))
        )
    levels.update(solve_tables(tuple(extent >> (LEVELS - 3) for extent in shape)))

    packed_shape = jax.ShapeDtypeStruct(
        (extents[0] // 2 * extents[1], 2 * extents[2]), jnp.float32
    )

    def gather(packed):
        copies = jnp.broadcast_to(packed[None], (devices,) + packed.shape)
        return lax.all_to_all(copies, ("gx", "gy", "gz"), 0, 0)

    def pack_body(tables_of, ins, outs):
        values = ins[0][...]
        outs[0][...] = pack(tables_of, values)
        lane = lax.broadcasted_iota(jnp.int32, block, 2)
        square = (block[0], block[1], block[1])
        same = lax.broadcasted_iota(jnp.int32, square, 1) == lax.broadcasted_iota(
            jnp.int32, square, 2
        )
        for out_ref, chosen in ((outs[1], block[2] - 1), (outs[2], 0)):
            face = jnp.sum(jnp.where(lane == chosen, values, 0.0), axis=2, keepdims=True)
            face = jnp.where(same, jnp.broadcast_to(face, square), 0.0)
            out_ref[...] = jnp.sum(face, axis=1, keepdims=True)

    kernel, arrays = with_tables(pack_body, own, 1)
    face_shape = jax.ShapeDtypeStruct((block[0], 1, block[1]), jnp.float32)
    packed, last_third, first_third = pl.pallas_call(
        kernel,
        out_shape=(packed_shape, face_shape, face_shape),
        in_specs=[vmem] * (1 + len(arrays)),
        out_specs=(vmem, vmem, vmem),
        name="pack",
    )(source, *arrays)

    def ring_shift(values, axis, step):
        count = lax.axis_size(axis)
        return lax.ppermute(values, axis, [(i, (i + step) % count) for i in range(count)])

    rims = [
        ring_shift(source[block[0] - 1 :], "gx", 1),
        ring_shift(source[:1], "gx", -1),
    ]
    last_second = source[:, block[1] - 1 :]
    first_second = source[:, :1]
    if counts[2] == 2:
        rims.append(ring_shift(jnp.stack([last_second, first_second]), "gz", 1))
    else:
        rims.append(
            jnp.stack([ring_shift(last_second, "gz", 1), ring_shift(first_second, "gz", -1)])
        )
    rims.append(ring_shift(last_third, "gy", 1))
    rims.append(ring_shift(first_third, "gy", -1))
    gathered = gather(packed)

    def first_body(tables_of, ins, outs):
        shift_ref, place_ref, gathered_ref, source_ref = ins[:4]
        low_first, high_first, both_second, low_third, high_third = ins[4:]
        packed_ref, iterate_ref, whole_ref, scratch_ref = outs
        shift_value = shift_ref[0]
        unpack(gathered_ref, whole_ref, counts, extents)
        whole_forcing = whole_ref[...]
        forcings = [whole_forcing]
        for grid_level in range(1, LEVELS - 2):
            fine = forcings[-1]
            coarse = down(tables_of, grid_level, fine)
            forcings.append(coarse.reshape(tuple(extent // 2 for extent in fine.shape)))
        iterate = solve_up(tables_of, "cubic", forcings[-1], shift_value)
        for grid_level in range(LEVELS - 2, 0, -1):
            forcing = forcings[grid_level - 1]
            if grid_level < LEVELS - 2:
                iterate = up(tables_of, grid_level, "cubic", flat(iterate), forcing.shape)
            iterate = vcycle_rolled(tables_of, grid_level, iterate, forcing, shift_value)
        window = own_window(iterate, scratch_ref, 3, extents, place_ref)
        iterate = from_right(flat(window), tables_of["own", "lanes_cubic"])
        iterate = from_left(tables_of["own", "rows_cubic"], iterate)
        iterate = iterate.reshape(block[0] + 4, rows_wide, lanes_wide)

        wide = (block[0], rows_wide, lanes_wide)
        row = lax.broadcasted_iota(jnp.int32, wide, 1)
        lane = lax.broadcasted_iota(jnp.int32, wide, 2)

        def widened(values):
            first = values.shape[0]
            values = jnp.concatenate([values, jnp.zeros_like(values[:, :8])], axis=1)
            return jnp.concatenate([values, jnp.zeros((first, rows_wide, block[2]))], axis=2)

        def rows_only(values):
            values = jnp.concatenate([values, jnp.zeros_like(values)], axis=2)
            return jnp.broadcast_to(values, wide)

        def lanes_only(values):
            square = (block[0], block[1], block[1])
            same = lax.broadcasted_iota(jnp.int32, square, 1) == lax.broadcasted_iota(
                jnp.int32, square, 2
            )
            values = jnp.where(same, jnp.broadcast_to(values, square), 0.0)
            values = jnp.sum(values, axis=2, keepdims=True)
            values = jnp.broadcast_to(values, (block[0], block[1], lanes_wide))
            return jnp.concatenate([values, jnp.zeros_like(values[:, :8])], axis=1)

        middle = widened(source_ref[...])
        middle = jnp.where(row == block[1], rows_only(both_second[1]), middle)
        middle = jnp.where(row == rows_wide - 1, rows_only(both_second[0]), middle)
        middle = jnp.where(lane == block[2], lanes_only(high_third[...]), middle)
        middle = jnp.where(lane == lanes_wide - 1, lanes_only(low_third[...]), middle)
        forcing = jnp.concatenate(
            [widened(low_first[...]), middle, widened(high_first[...])], axis=0
        )
        diagonal = 6.0 + shift_value
        iterate = sweep_rolled(iterate, forcing, 1.0, diagonal, False)
        iterate_ref[...] = iterate
        residue = defect_rolled(iterate, middle, 1.0, diagonal, False)
        packed_ref[...] = pack(tables_of, residue[:, : block[1], : block[2]])

    tables_map = {**levels, **own, **edge_tables("cubic", CUBIC_EVEN, CUBIC_ODD, 2)}
    kernel, arrays = with_tables(first_body, tables_map, 9)
    iterate_shape = jax.ShapeDtypeStruct((block[0] + 2, rows_wide, lanes_wide), jnp.float32)
    packed, iterate = pl.pallas_call(
        kernel,
        out_shape=(packed_shape, iterate_shape),
        in_specs=[smem, smem] + [vmem] * (7 + len(arrays)),
        out_specs=(vmem, vmem),
        scratch_shapes=[
            pltpu.VMEM(shape, jnp.float32),
            pltpu.VMEM((shape[0] + 6, *shape[1:]), jnp.float32),
        ],
        name="first",
    )(shift, place, gathered, source, *rims, *arrays)
    gathered = gather(packed)

    def second_body(tables_of, ins, outs):
        shift_ref, place_ref, gathered_ref, source_ref, iterate_ref = ins
        result_ref, whole_ref, scratch_ref = outs
        shift_value = shift_ref[0]
        unpack(gathered_ref, whole_ref, counts, extents)
        correction = vcycle_rolled(tables_of, 1, None, whole_ref[...], shift_value)
        window = own_window(correction, scratch_ref, 2, extents, place_ref)
        wide = from_right(flat(window), tables_of["own", "lanes_linear"])
        wide = from_left(tables_of["own", "rows_linear"], wide).reshape(iterate_shape.shape)
        iterate = iterate_ref[...] + wide
        center, total = beside_rolled(iterate, False)
        center = center[:, : block[1], : block[2]]
        total = total[:, : block[1], : block[2]]
        diagonal = 6.0 + shift_value
        scale = damping_over(diagonal, block[2])
        result_ref[...] = center + scale * (source_ref[...] - (diagonal * center - total))

    tables_map = {key: value for key, value in levels.items() if "cubic" not in key[1]}
    tables_map.update(edge_tables("linear", LINEAR_EVEN, LINEAR_ODD, 1))
    kernel, arrays = with_tables(second_body, tables_map, 5)
    return pl.pallas_call(
        kernel,
        out_shape=jax.ShapeDtypeStruct(block, jnp.float32),
        in_specs=[smem, smem] + [vmem] * (3 + len(arrays)),
        out_specs=vmem,
        scratch_shapes=[
            pltpu.VMEM(shape, jnp.float32),
            pltpu.VMEM((shape[0] + 4, *shape[1:]), jnp.float32),
        ],
        name="second",
    )(shift, place, gathered, source, iterate, *arrays)


WHOLE_LIMIT = 1 << 18


def per_device(source, shift):
    block = source.shape
    counts = tuple(lax.axis_size(axis) for axis in ("gx", "gy", "gz"))
    cells = math.prod(block) // 8 * math.prod(counts)
    second_deep = block[1] * counts[2] >> (LEVELS - 2)
    third_deep = block[2] * counts[1] >> (LEVELS - 2)
    aligned = (
        block[0] % 4 == 0
        and block[1] % 16 == 0
        and block[2] == 128
        and counts[1] % 2 == 0
        and second_deep % 8 == 0
        and third_deep % 128 == 0
        and block[0] * counts[0] >= 32
    )
    if aligned and cells <= WHOLE_LIMIT:
        return per_device_kernels(source, shift)
    return per_device_plain(source, shift)


def solution(mesh):
    in_specs = (P("gx", "gz", "gy"), P())
    out_specs = P("gx", "gz", "gy")
    return jax.shard_map(
        per_device, mesh=mesh, in_specs=in_specs, out_specs=out_specs, check_vma=False
    )
```
